32 devices in a mesh: batch: 1 (over z), dap: 32 (over y, x, core).
Axes of the slice: x: 4, y: 4, z: 1, core: 2. Of those that a mesh axis runs over, the one named last changes fastest.
The devices are a block of a 4x4x8 slice.
Arguments:
- pair: bfloat16 [512, 512, 128], P(('batch', 'dap'))
- pair_mask: int32 [512, 512], P(('batch', 'dap'))
- ln_in: bfloat16 [2, 2, 128], replicated
- w_proj: bfloat16 [2, 128, 512], replicated
- b_proj: bfloat16 [2, 512], replicated
- w_gate: bfloat16 [2, 128, 128], replicated
- b_gate: bfloat16 [2, 128], replicated
- ln_out: bfloat16 [2, 2, 128], replicated
- w_out: bfloat16 [2, 128, 128], replicated
- b_out: bfloat16 [2, 128], replicated
Outputs:
- output: bfloat16 [512, 512, 128], P(('batch', 'dap'))
All inputs are finite; a program needn't handle non-finite values.
Results may differ from the reference program's by a relative error of at most 0.00381369.
Values are sent between devices in bfloat16 or wider.
A program may use at most 768 MiB of HBM per device.

```python
import jax
import jax.numpy as jnp
from jax import lax

N = 512
CZ = 128
CH = 128
LN_EPS = 1e-5


def setup_inputs(seed: int = 0, part: int = 0) -> dict:
    base_key = jax.random.key(seed)
    part_key = jax.random.fold_in(base_key, part)
    pair_key, mask_key = jax.random.split(part_key)
    weight_keys = jax.random.split(jax.random.fold_in(base_key, 1000), 10)
    pair = jax.random.normal(pair_key, (N, N, CZ), jnp.float32)
    pair_mask = (jax.random.randint(mask_key, (N, N), 0, 8) > 0).astype(jnp.int32)
    ln_in = jnp.stack([1.0 + 0.3 * jax.random.normal(weight_keys[0], (2, CZ), jnp.float32),
                       0.3 * jax.random.normal(weight_keys[1], (2, CZ), jnp.float32)], axis=1)
    w_proj = jax.random.normal(weight_keys[2], (2, CZ, 4 * CH), jnp.float32) * CZ ** -0.5
    b_proj = 0.5 * jax.random.normal(weight_keys[3], (2, 4 * CH), jnp.float32)
    w_gate = jax.random.normal(weight_keys[4], (2, CZ, CZ), jnp.float32) * CZ ** -0.5
    b_gate = 0.5 * jax.random.normal(weight_keys[5], (2, CZ), jnp.float32)
    ln_out = jnp.stack([1.0 + 0.3 * jax.random.normal(weight_keys[6], (2, CH), jnp.float32),
                        0.3 * jax.random.normal(weight_keys[7], (2, CH), jnp.float32)], axis=1)
    w_out = jax.random.normal(weight_keys[8], (2, CH, CZ), jnp.float32) * CH ** -0.5
    b_out = 0.5 * jax.random.normal(weight_keys[9], (2, CZ), jnp.float32)
    return {
        "pair": pair.astype(jnp.bfloat16),
        "pair_mask": pair_mask,
        "ln_in": ln_in.astype(jnp.bfloat16),
        "w_proj": w_proj.astype(jnp.bfloat16),
        "b_proj": b_proj.astype(jnp.bfloat16),
        "w_gate": w_gate.astype(jnp.bfloat16),
        "b_gate": b_gate.astype(jnp.bfloat16),
        "ln_out": ln_out.astype(jnp.bfloat16),
        "w_out": w_out.astype(jnp.bfloat16),
        "b_out": b_out.astype(jnp.bfloat16),
    }


def layer_norm(values, scale, offset):
    centred = values - jnp.mean(values, axis=-1, keepdims=True)
    variance = jnp.mean(centred * centred, axis=-1, keepdims=True)
    return centred * lax.rsqrt(variance + LN_EPS) * scale.astype(jnp.float32) + offset.astype(jnp.float32)


def channel_product(left, right, contract_form):
    groups = CH // 16
    left_groups = jnp.moveaxis(left.reshape(N, N, groups, 16), 2, 0)
    right_groups = jnp.moveaxis(right.reshape(N, N, groups, 16), 2, 0)

    def group_sum(operands):
        return jnp.einsum(contract_form, operands[0].astype(jnp.float32), operands[1].astype(jnp.float32))

    summed = lax.map(group_sum, (left_groups, right_groups))
    return jnp.moveaxis(summed, 0, 2).reshape(N, N, CH)


def tri_layer(pair, keep_mask, ln_in, w_proj, b_proj, w_gate, b_gate, ln_out, w_out, b_out, contract_form):
    row_blocks = N // 8

    def make_sides(operands):
        block, mask_block = operands
        normed = layer_norm(block.astype(jnp.float32), ln_in[0], ln_in[1]).astype(jnp.bfloat16)
        projected = jnp.dot(normed.reshape(8 * N, CZ), w_proj, preferred_element_type=jnp.float32)
        projected = (projected + b_proj.astype(jnp.float32)).reshape(8, N, 4 * CH)
        left = mask_block * jax.nn.sigmoid(projected[..., CH:2 * CH]) * projected[..., :CH]
        right = mask_block * jax.nn.sigmoid(projected[..., 3 * CH:]) * projected[..., 2 * CH:3 * CH]
        return normed, left.astype(jnp.bfloat16), right.astype(jnp.bfloat16)

    pair_blocks = pair.reshape(row_blocks, 8, N, CZ)
    normed, left, right = lax.map(make_sides, (pair_blocks, keep_mask.reshape(row_blocks, 8, N, 1)))
    tri_sum = channel_product(left.reshape(N, N, CH), right.reshape(N, N, CH), contract_form)

    def finish(operands):
        block, normed_block, tri_block = operands
        tri_norm = layer_norm(tri_block, ln_out[0], ln_out[1]).astype(jnp.bfloat16)
        update = jnp.dot(tri_norm.reshape(8 * N, CH), w_out, preferred_element_type=jnp.float32) + b_out.astype(jnp.float32)
        gates = jax.nn.sigmoid(jnp.dot(normed_block.reshape(8 * N, CZ), w_gate, preferred_element_type=jnp.float32) + b_gate.astype(jnp.float32))
        return (block.astype(jnp.float32) + (gates * update).reshape(8, N, CZ)).astype(jnp.bfloat16)

    result = lax.map(finish, (pair_blocks, normed, tri_sum.reshape(row_blocks, 8, N, CH)))
    return result.reshape(N, N, CZ)


def reference(pair, pair_mask, ln_in, w_proj, b_proj, w_gate, b_gate, ln_out, w_out, b_out):
    keep_mask = pair_mask.astype(jnp.float32)[..., None]
    first = tri_layer(pair, keep_mask, ln_in[0], w_proj[0], b_proj[0], w_gate[0], b_gate[0],
                      ln_out[0], w_out[0], b_out[0], "ikc,jkc->ijc")
    return tri_layer(first, keep_mask, ln_in[1], w_proj[1], b_proj[1], w_gate[1], b_gate[1],
                     ln_out[1], w_out[1], b_out[1], "kic,kjc->ijc")
```

```python
import functools
import math

import jax
import jax.numpy as jnp
from jax import lax
from jax.experimental import pallas as pl
from jax.experimental.pallas import tpu as pltpu
from jax.sharding import PartitionSpec as P

LN_EPS = 1e-5
LANES = 128
MESH = pl.DeviceIdType.MESH
F32 = jnp.float32
BF16 = jnp.bfloat16


def send_order(side):
    near = [(1, 0), (-1, 0), (0, 1), (0, -1), (2, 0), (0, 2), (1, 1), (-1, -1), (1, -1), (-1, 1), (2, 2), (1, 2),
            (-1, 2), (2, 1), (2, -1), (0, 0)]
    found, order = set(), []
    for dc in range(2):
        for dx, dy in near + [(x, y) for x in range(side) for y in range(side)]:
            offset = (dy % side, dx % side, dc)
            if offset not in found and offset != (0, 0, 0):
                found.add(offset)
                order.append(offset)
    return order


def dot(left, right, dims):
    return lax.dot_general(left, right, (dims, ((), ())), preferred_element_type=F32)


def norm_rows(values, scale, offset):
    count = values.shape[0]
    centred = values - jnp.sum(values, axis=0, keepdims=True) * (1.0 / count)
    variance = jnp.sum(centred * centred, axis=0, keepdims=True) * (1.0 / count)
    return (centred * lax.rsqrt(variance + LN_EPS) * scale + offset).astype(BF16)


def kernel(n, side, slots, pitch, z_ref, mask_ref, wp_ref, bp_ref, wg_ref, wo_ref, vec_ref, out_ref,
           ab_send, ab_recv, o_send, o_recv, stage_a, stage_b, zt, znt, gate, ssem, rsem):
    rows, cols, channels = z_ref.shape
    tiles = cols // LANES
    order = send_order(side)
    me = lax.axis_index("dap")
    core, place = lax.rem(me, 2), me // 2
    my_x, my_y = lax.rem(place, side), place // side

    barrier = pltpu.get_barrier_semaphore()
    for step in range(1, n):
        pl.semaphore_signal(barrier, inc=1, device_id={"dap": lax.rem(me + step, n)}, device_id_type=MESH)

    def peers():
        for dy, dx, dc in order:
            y, x, c = lax.rem(my_y + dy, side), lax.rem(my_x + dx, side), lax.rem(core + dc, 2)
            yield (y * side + x) * 2 + c

    def send_sides(layer, slot):
        target = ab_recv.at[layer, slot, :, pl.ds(pl.multiple_of(me * rows, rows), rows), :]
        phase = 2 * layer
        for peer in peers():
            pltpu.make_async_remote_copy(ab_send.at[slot, peer], target, ssem.at[phase, slot], rsem.at[phase, slot],
                                         device_id={"dap": peer}, device_id_type=MESH).start()
        pltpu.make_async_copy(ab_send.at[slot, me], target, rsem.at[phase, slot]).start()

    def send_sums(layer, slot):
        target = o_recv.at[:, pl.ds(pl.multiple_of((slot * n + me) * pitch, 8), rows), :]
        phase = 2 * layer + 1
        for peer in peers():
            source = o_send.at[slot, :, pl.ds(pl.multiple_of(peer * rows, rows), rows), :]
            pltpu.make_async_remote_copy(source, target, ssem.at[phase, slot], rsem.at[phase, slot],
                                         device_id={"dap": peer}, device_id_type=MESH).start()
        source = o_send.at[slot, :, pl.ds(pl.multiple_of(me * rows, rows), rows), :]
        pltpu.make_async_copy(source, target, rsem.at[phase, slot]).start()

    def wait_bytes(ref, sem):
        pltpu.make_async_copy(ref, ref, sem).wait()

    def wait_sides_sent(layer, slot):
        wait_bytes(ab_send.at[slot, pl.ds(0, n - 1)], ssem.at[2 * layer, slot])

    def wait_sums_sent(layer, slot):
        wait_bytes(o_send.at[slot, :, pl.ds(0, (n - 1) * rows), :], ssem.at[2 * layer + 1, slot])

    def wait_sides(layer, slot):
        wait_bytes(ab_recv.at[layer, slot], rsem.at[2 * layer, slot])

    def wait_sums(layer, slot):
        wait_bytes(o_send.at[slot], rsem.at[2 * layer + 1, slot])

    def make_sides(layer, slot):
        weight = wp_ref[layer, slot]
        bias = bp_ref[layer, slot]

        def row(i, carry):
            projected = dot(weight, znt[i], ((1,), (0,))) + bias
            keep = mask_ref[pl.ds(i, 1), :].astype(F32)
            left = keep * jax.nn.sigmoid(projected[n:2 * n]) * projected[:n]
            right = keep * jax.nn.sigmoid(projected[3 * n:]) * projected[2 * n:3 * n]
            for t in range(tiles):
                stage_a[t, pl.ds(i, n, stride=pitch), :] = left[:, t * LANES:(t + 1) * LANES]
                stage_b[t, pl.ds(i, n, stride=pitch), :] = right[:, t * LANES:(t + 1) * LANES]
            return carry

        lax.fori_loop(0, rows, row, 0)

        def pack(d, carry):
            start = pl.multiple_of(d * pitch, 8)
            for t in range(tiles):
                ab_send[slot, d, 0, :, t * LANES:(t + 1) * LANES] = stage_a[t, pl.ds(start, rows), :].astype(BF16)
                ab_send[slot, d, 1, :, t * LANES:(t + 1) * LANES] = stage_b[t, pl.ds(start, rows), :].astype(BF16)
            return carry

        lax.fori_loop(0, n, pack, 0)

    def make_gates(layer):
        def row(i, carry):
            gate[i] = jax.nn.sigmoid(dot(wg_ref[layer], znt[i], ((1,), (0,))) + vec_ref[layer, 2])
            return carry

        lax.fori_loop(0, rows, row, 0)

    def triangle(layer, slot):
        if layer == 0:
            left = ab_recv[0, slot, 0]
            dims = ((1,), (1,))
        else:
            left = ab_recv[1, slot, 0].T
            dims = ((1,), (0,))
        for t in range(tiles):
            if layer == 0:
                right = ab_recv[0, slot, 1, t * LANES:(t + 1) * LANES, :]
            else:
                right = ab_recv[1, slot, 1, :, t * LANES:(t + 1) * LANES]
            o_send[slot, t] = dot(left, right, dims)

    def finish(layer):
        def row(i, carry):
            for t in range(tiles):
                part = slice(t * LANES, (t + 1) * LANES)
                u = norm_rows(o_recv[t, pl.ds(i, channels, stride=pitch), :], vec_ref[layer, 3], vec_ref[layer, 4])
                update = dot(wo_ref[layer], u, ((1,), (0,))) + vec_ref[layer, 5]
                new = (zt[i, :, part].astype(F32) + gate[i, :, part] * update).astype(BF16)
                if layer == 0:
                    zt[i, :, part] = new
                    znt[i, :, part] = norm_rows(new.astype(F32), vec_ref[1, 0], vec_ref[1, 1])
                else:
                    out_ref[i, part, :] = new.astype(F32).T.astype(BF16)
            return carry

        lax.fori_loop(0, rows, row, 0)

    def first_norm(i, carry):
        values = z_ref[i].astype(F32).T
        zt[i] = values.astype(BF16)
        znt[i] = norm_rows(values, vec_ref[0, 0], vec_ref[0, 1])
        return carry

    lax.fori_loop(0, rows, first_norm, 0)

    for layer in range(2):
        def give_sides(slot, carry):
            if layer == 1:
                wait_sides_sent(0, slot)
            make_sides(layer, slot)
            if layer == 0:
                @pl.when(slot == 0)
                def _():
                    pl.semaphore_wait(barrier, n - 1)
            send_sides(layer, slot)
            return carry

        def give_sums(slot, carry):
            wait_sides(layer, slot)
            if layer == 1:
                wait_sums_sent(0, slot)
            triangle(layer, slot)
            send_sums(layer, slot)
            return carry

        lax.fori_loop(0, slots, give_sides, 0)
        make_gates(layer)
        lax.fori_loop(0, slots, give_sums, 0)
        lax.fori_loop(0, slots, lambda slot, carry: (wait_sums(layer, slot), carry)[1], 0)
        finish(layer)

    def drain(slot, carry):
        wait_sides_sent(1, slot)
        wait_sums_sent(1, slot)
        return carry

    lax.fori_loop(0, slots, drain, 0)


def solution(mesh):
    n = mesh.shape["dap"]
    side = math.isqrt(n // 2)
    row_spec = P(("batch", "dap"), None, None)
    mask_spec = P(("batch", "dap"), None)

    def local_layers(pair, pair_mask, ln_in, w_proj, b_proj, w_gate, b_gate, ln_out, w_out, b_out):
        rows, cols, channels = pair.shape
        slots = channels // n
        tiles = cols // LANES
        pitch = rows + 8
        layers = w_proj.shape[0]

        def by_slot(array):
            split = array.reshape((layers, 4, slots, n) + array.shape[2:])
            return jnp.swapaxes(split, 1, 2).reshape((layers, slots, 4 * n) + array.shape[2:])

        wp = by_slot(jnp.swapaxes(w_proj, 1, 2))
        bp = by_slot(b_proj[..., None]).astype(F32)
        vec = jnp.stack([ln_in[:, 0], ln_in[:, 1], b_gate, ln_out[:, 0], ln_out[:, 1], b_out], axis=1)[..., None].astype(F32)
        vmem = pl.BlockSpec(memory_space=pltpu.VMEM)
        return pl.pallas_call(
            functools.partial(kernel, n, side, slots, pitch),
            out_shape=jax.ShapeDtypeStruct(pair.shape, BF16),
            in_specs=[vmem] * 7,
            out_specs=vmem,
            scratch_shapes=[
                pltpu.VMEM((slots, n, 2, rows, cols), BF16),
                pltpu.VMEM((2, slots, 2, cols, cols), BF16),
                pltpu.VMEM((slots, tiles, cols, LANES), F32),
                pltpu.VMEM((tiles, channels * pitch, LANES), F32),
                pltpu.VMEM((tiles, n * pitch, LANES), F32),
                pltpu.VMEM((tiles, n * pitch, LANES), F32),
                pltpu.VMEM((rows, channels, cols), BF16),
                pltpu.VMEM((rows, channels, cols), BF16),
                pltpu.VMEM((rows, channels, cols), F32),
                pltpu.SemaphoreType.DMA((4, slots)),
                pltpu.SemaphoreType.DMA((4, slots)),
            ],
            compiler_params=pltpu.CompilerParams(collective_id=0, has_side_effects=True, vmem_limit_bytes=60 * 2 ** 20),
            name="triangle_pair",
        )(pair, pair_mask, wp, bp, jnp.swapaxes(w_gate, 1, 2), jnp.swapaxes(w_out, 1, 2), vec)

    return jax.shard_map(local_layers, mesh=mesh,
                         in_specs=(row_spec, mask_spec, P(), P(), P(), P(), P(), P(), P(), P()),
                         out_specs=row_spec, check_vma=False)
```

```python
import functools
import math

import jax
import jax.numpy as jnp
from jax import lax
from jax.experimental import pallas as pl
from jax.experimental.pallas import tpu as pltpu
from jax.sharding import PartitionSpec as P

LN_EPS = 1e-5
LANES = 128
MESH = pl.DeviceIdType.MESH
F32 = jnp.float32
BF16 = jnp.bfloat16


def send_order(side):
    near = [(1, 0), (-1, 0), (0, 1), (0, -1), (2, 0), (0, 2), (1, 1), (-1, -1), (1, -1), (-1, 1), (2, 2), (1, 2),
            (-1, 2), (2, 1), (2, -1), (0, 0)]
    found, order = set(), []
    for dc in range(2):
        for dx, dy in near + [(x, y) for x in range(side) for y in range(side)]:
            offset = (dy % side, dx % side, dc)
            if offset not in found and offset != (0, 0, 0):
                found.add(offset)
                order.append(offset)
    return order


def dot(left, right, dims):
    return lax.dot_general(left, right, (dims, ((), ())), preferred_element_type=F32)


def norm_rows(values, scale, offset):
    count = values.shape[0]
    centred = values - jnp.sum(values, axis=0, keepdims=True) * (1.0 / count)
    variance = jnp.sum(centred * centred, axis=0, keepdims=True) * (1.0 / count)
    return (centred * lax.rsqrt(variance + LN_EPS) * scale + offset).astype(BF16)


def kernel(n, side, slots, pitch, z_ref, mask_ref, ln_in_ref, w_proj_ref, b_proj_ref, w_gate_ref, b_gate_ref, ln_out_ref,
           w_out_ref, b_out_ref, out_ref, ab_send, ab_recv, o_send, o_recv, stage_a, stage_b, turned, zt, znt, gate,
           wp, bp, wg, wo, vec, keep, ssem, rsem, ssem_part, rsem_part):
    rows, cols, channels = z_ref.shape
    tiles = cols // LANES
    group = 4
    order = send_order(side)
    me = lax.axis_index("dap")
    core, place = lax.rem(me, 2), me // 2
    my_x, my_y = lax.rem(place, side), place // side
    my_rows = pl.ds(pl.multiple_of(me * rows, rows), rows)

    barrier = pltpu.get_barrier_semaphore()
    for step in range(1, n):
        pl.semaphore_signal(barrier, inc=1, device_id={"dap": lax.rem(me + step, n)}, device_id_type=MESH)

    def lanes(t):
        return pl.ds(pl.multiple_of(t * LANES, LANES), LANES)

    def loop(count, body):
        def step(index, carry):
            body(index)
            return carry

        lax.fori_loop(0, count, step, 0)

    def send_all(source_of, target, send_sem, recv_sem):
        for dy, dx, dc in order:
            y, x, c = lax.rem(my_y + dy, side), lax.rem(my_x + dx, side), lax.rem(core + dc, 2)
            peer = (y * side + x) * 2 + c
            pltpu.make_async_remote_copy(source_of(peer), target, send_sem, recv_sem,
                                         device_id={"dap": peer}, device_id_type=MESH).start()
        pltpu.make_async_copy(source_of(me), target, recv_sem).start()

    def wait_bytes(ref, sem):
        pltpu.make_async_copy(ref, ref, sem).wait()

    def send_sides(layer, slot):
        send_all(lambda peer: ab_send.at[slot, peer], ab_recv.at[layer, slot, :, my_rows, :],
                 ssem.at[2 * layer, slot], rsem.at[2 * layer, slot])

    def send_sides_part(layer, t):
        send_all(lambda peer: ab_send.at[0, peer, :, :, lanes(t)], ab_recv.at[layer, 0, :, my_rows, lanes(t)],
                 ssem_part.at[2 * layer, t], rsem_part.at[2 * layer, t])

    def wait_sides(layer, slot):
        wait_bytes(ab_recv.at[layer, slot], rsem.at[2 * layer, slot])

    def wait_sides_part(layer, t):
        wait_bytes(ab_recv.at[layer, 0, :, :, lanes(t)], rsem_part.at[2 * layer, t])

    def wait_sides_sent(layer, slot):
        wait_bytes(ab_send.at[slot, pl.ds(0, n - 1)], ssem.at[2 * layer, slot])

    def wait_sides_sent_part(layer, t):
        wait_bytes(ab_send.at[0, pl.ds(0, n - 1), :, :, lanes(t)], ssem_part.at[2 * layer, t])

    def sum_rows(device):
        return pl.ds(pl.multiple_of(device * rows, rows), rows)

    def sum_target(slot):
        return pl.ds(pl.multiple_of((slot * n + me) * pitch, 8), rows)

    def send_sums(layer, slot):
        send_all(lambda peer: o_send.at[slot, :, sum_rows(peer), :], o_recv.at[:, sum_target(slot), :],
                 ssem.at[2 * layer + 1, slot], rsem.at[2 * layer + 1, slot])

    def send_sums_part(layer, t):
        send_all(lambda peer: o_send.at[slots - 1, t, sum_rows(peer), :], o_recv.at[t, sum_target(slots - 1), :],
                 ssem_part.at[2 * layer + 1, t], rsem_part.at[2 * layer + 1, t])

    def wait_sums(layer, slot):
        wait_bytes(o_send.at[slot], rsem.at[2 * layer + 1, slot])

    def wait_sums_part(layer, t):
        wait_bytes(o_send.at[slots - 1, t], rsem_part.at[2 * layer + 1, t])

    def wait_sums_sent(layer, slot):
        wait_bytes(o_send.at[slot, :, pl.ds(0, (n - 1) * rows), :], ssem.at[2 * layer + 1, slot])

    def wait_sums_sent_part(layer, t):
        wait_bytes(o_send.at[slots - 1, t, pl.ds(0, (n - 1) * rows), :], ssem_part.at[2 * layer + 1, t])

    def column(row):
        return jnp.broadcast_to(row.astype(F32), (LANES, row.shape[-1])).T

    def prepare_first(layer):
        for block in range(4):
            part = slice(block * channels, (block + 1) * channels)
            weight = w_proj_ref[layer, :, part].astype(F32).T.astype(BF16)
            bias = column(b_proj_ref[layer:layer + 1, part])
            for slot in range(slots):
                wp[layer, slot, block * n:(block + 1) * n] = weight[slot * n:(slot + 1) * n]
                bp[layer, slot, block * n:(block + 1) * n] = bias[slot * n:(slot + 1) * n]
        vec[layer, 0] = column(ln_in_ref[layer, 0:1])
        vec[layer, 1] = column(ln_in_ref[layer, 1:2])

    def prepare_rest(layer):
        wg[layer] = w_gate_ref[layer].astype(F32).T.astype(BF16)
        wo[layer] = w_out_ref[layer].astype(F32).T.astype(BF16)
        vec[layer, 2] = column(b_gate_ref[layer:layer + 1])
        vec[layer, 3] = column(ln_out_ref[layer, 0:1])
        vec[layer, 4] = column(ln_out_ref[layer, 1:2])
        vec[layer, 5] = column(b_out_ref[layer:layer + 1])

    def first_norm(t):
        def some(step):
            for k in range(group):
                i = step * group + k
                values = z_ref[i, lanes(t), :].astype(F32).T
                zt[i, :, lanes(t)] = values.astype(BF16)
                znt[i, :, lanes(t)] = norm_rows(values, vec[0, 0], vec[0, 1])

        loop(rows // group, some)

    def gated(layer, slot, pairs):
        normed = jnp.concatenate([znt[i, :, lanes(t)] for i, t in pairs], axis=1)
        projected = dot(wp[layer, slot], normed, ((1,), (0,)))
        bias = bp[layer, slot]
        for k, (i, t) in enumerate(pairs):
            part = projected[:, k * LANES:(k + 1) * LANES] + bias
            kept = keep[t, pl.ds(i, 1), :]
            stage_a[t, pl.ds(i, n, stride=pitch), :] = kept * jax.nn.sigmoid(part[n:2 * n]) * part[:n]
            stage_b[t, pl.ds(i, n, stride=pitch), :] = kept * jax.nn.sigmoid(part[3 * n:]) * part[2 * n:3 * n]

    def pack(slot, tile_list, unroll):
        def some(step):
            for k in range(unroll):
                d = step * unroll + k
                start = pl.multiple_of(d * pitch, 8)
                for t in tile_list:
                    ab_send[slot, d, 0, :, lanes(t)] = stage_a[t, pl.ds(start, rows), :].astype(BF16)
                    ab_send[slot, d, 1, :, lanes(t)] = stage_b[t, pl.ds(start, rows), :].astype(BF16)

        loop(n // unroll, some)

    def make_sides(layer, slot):
        loop(rows, lambda i: gated(layer, slot, [(i, t) for t in range(tiles)]))
        pack(slot, range(tiles), 1)

    def make_sides_part(layer, t):
        loop(rows // group, lambda step: gated(layer, 0, [(step * group + k, t) for k in range(group)]))
        pack(0, [t], 4)

    def make_gates(layer):
        def row(i):
            projected = dot(wg[layer], znt[i], ((1,), (0,)))
            for t in range(tiles):
                part = slice(t * LANES, (t + 1) * LANES)
                gate[i, :, part] = jax.nn.sigmoid(projected[:, part] + vec[layer, 2])

        loop(rows, row)

    def turn(layer, slot):
        if layer == 1:
            turned[...] = ab_recv[1, slot, 0].T

    def triangle(layer, slot, t):
        if layer == 0:
            o_send[slot, t] = dot(ab_recv[0, slot, 0], ab_recv[0, slot, 1, lanes(t), :], ((1,), (1,)))
        else:
            o_send[slot, t] = dot(turned[...], ab_recv[1, slot, 1, :, lanes(t)], ((1,), (0,)))

    def finish(layer, t):
        def some(step):
            places = [step * group + k for k in range(group)]
            normed = [norm_rows(o_recv[t, pl.ds(i, channels, stride=pitch), :], vec[layer, 3], vec[layer, 4]) for i in places]
            update = dot(wo[layer], jnp.concatenate(normed, axis=1), ((1,), (0,)))
            for k, i in enumerate(places):
                added = update[:, k * LANES:(k + 1) * LANES] + vec[layer, 5]
                new = (zt[i, :, lanes(t)].astype(F32) + gate[i, :, lanes(t)] * added).astype(BF16)
                if layer == 0:
                    zt[i, :, lanes(t)] = new
                    znt[i, :, lanes(t)] = norm_rows(new.astype(F32), vec[1, 0], vec[1, 1])
                else:
                    out_ref[i, :, lanes(t)] = new

        loop(rows // group, some)

    prepare_first(0)
    for t in range(tiles):
        keep[t] = mask_ref[:, t * LANES:(t + 1) * LANES].astype(F32)

    def start(t):
        first_norm(t)
        make_sides_part(0, t)

        @pl.when(t == 0)
        def _():
            pl.semaphore_wait(barrier, n - 1)

        send_sides_part(0, t)

    loop(tiles, start)
    for layer in range(2):
        def give_sides(step):
            if layer == 1:
                wait_sides_sent(0, step + 1)
            make_sides(layer, step + 1)
            send_sides(layer, step + 1)

        def give_sums(slot):
            @pl.when(slot == 0)
            def _():
                loop(tiles, lambda t: wait_sides_part(layer, t))

            @pl.when(slot > 0)
            def _():
                wait_sides(layer, slot)

            if layer == 1:
                wait_sums_sent(0, slot)
            turn(layer, slot)
            loop(tiles, lambda t: triangle(layer, slot, t))
            send_sums(layer, slot)

        def give_last_sums(t):
            if layer == 1:
                wait_sums_sent_part(0, t)
            triangle(layer, slots - 1, t)
            send_sums_part(layer, t)

        def take_sums(t):
            wait_sums_part(layer, t)
            finish(layer, t)
            if layer == 0:
                wait_sides_sent_part(0, t)
                make_sides_part(1, t)
                send_sides_part(1, t)

        loop(slots - 1, give_sides)
        if layer == 0:
            prepare_rest(0)
            prepare_first(1)
            prepare_rest(1)
        make_gates(layer)
        loop(slots - 1, give_sums)
        wait_sides(layer, slots - 1)
        turn(layer, slots - 1)
        loop(tiles, give_last_sums)
        loop(slots - 1, lambda slot: wait_sums(layer, slot))
        loop(tiles, take_sums)

    def drain(step):
        wait_sides_sent(1, step + 1)
        wait_sums_sent(1, step)

    def drain_part(t):
        wait_sides_sent_part(1, t)
        wait_sums_sent_part(1, t)

    loop(slots - 1, drain)
    loop(tiles, drain_part)


def solution(mesh):
    n = mesh.shape["dap"]
    side = math.isqrt(n // 2)
    row_spec = P(("batch", "dap"), None, None)
    mask_spec = P(("batch", "dap"), None)

    def local_layers(pair, *others):
        rows, cols, channels = pair.shape
        slots = channels // n
        tiles = cols // LANES
        pitch = rows + 8
        vmem = pl.BlockSpec(memory_space=pltpu.VMEM)
        turned_out = pl.pallas_call(
            functools.partial(kernel, n, side, slots, pitch),
            out_shape=jax.ShapeDtypeStruct((rows, channels, cols), BF16),
            in_specs=[vmem] * (1 + len(others)),
            out_specs=vmem,
            scratch_shapes=[
                pltpu.VMEM((slots, n, 2, rows, cols), BF16),
                pltpu.VMEM((2, slots, 2, cols, cols), BF16),
                pltpu.VMEM((slots, tiles, cols, LANES), F32),
                pltpu.VMEM((tiles, channels * pitch, LANES), F32),
                pltpu.VMEM((tiles, n * pitch, LANES), F32),
                pltpu.VMEM((tiles, n * pitch, LANES), F32),
                pltpu.VMEM((cols, cols), BF16),
                pltpu.VMEM((rows, channels, cols), BF16),
                pltpu.VMEM((rows, channels, cols), BF16),
                pltpu.VMEM((rows, channels, cols), F32),
                pltpu.VMEM((2, slots, 4 * n, channels), BF16),
                pltpu.VMEM((2, slots, 4 * n, LANES), F32),
                pltpu.VMEM((2, channels, channels), BF16),
                pltpu.VMEM((2, channels, channels), BF16),
                pltpu.VMEM((2, 6, channels, LANES), F32),
                pltpu.VMEM((tiles, rows, LANES), F32),
                pltpu.SemaphoreType.DMA((4, slots)),
                pltpu.SemaphoreType.DMA((4, slots)),
                pltpu.SemaphoreType.DMA((4, tiles)),
                pltpu.SemaphoreType.DMA((4, tiles)),
            ],
            compiler_params=pltpu.CompilerParams(collective_id=0, has_side_effects=True, vmem_limit_bytes=60 * 2 ** 20),
            name="triangle_pair",
        )(pair, *others)
        return jnp.swapaxes(turned_out, 1, 2)

    return jax.shard_map(local_layers, mesh=mesh,
                         in_specs=(row_spec, mask_spec, P(), P(), P(), P(), P(), P(), P(), P()),
                         out_specs=row_spec, check_vma=False)
```

```python
import functools
import math

import jax
import jax.numpy as jnp
from jax import lax
from jax.experimental import pallas as pl
from jax.experimental.pallas import tpu as pltpu
from jax.sharding import PartitionSpec as P

LN_EPS = 1e-5
LANES = 128
MESH = pl.DeviceIdType.MESH
F32 = jnp.float32
BF16 = jnp.bfloat16


def send_order(side):
    near = [(1, 0), (-1, 0), (0, 1), (0, -1), (2, 0), (0, 2), (1, 1), (-1, -1), (1, -1), (-1, 1), (2, 2), (1, 2),
            (-1, 2), (2, 1), (2, -1), (0, 0)]
    found, order = set(), []
    for dc in range(2):
        for dx, dy in near + [(x, y) for x in range(side) for y in range(side)]:
            offset = (dy % side, dx % side, dc)
            if offset not in found and offset != (0, 0, 0):
                found.add(offset)
                order.append(offset)
    return order


def dot(left, right, dims):
    return lax.dot_general(left, right, (dims, ((), ())), preferred_element_type=F32)


def norm_rows(values, scale, offset):
    count = values.shape[0]
    centred = values - jnp.sum(values, axis=0, keepdims=True) * (1.0 / count)
    variance = jnp.sum(centred * centred, axis=0, keepdims=True) * (1.0 / count)
    return (centred * lax.rsqrt(variance + LN_EPS) * scale + offset).astype(BF16)


def kernel(n, side, slots, pitch, z_ref, mask_ref, ln_in_ref, w_proj_ref, b_proj_ref, w_gate_ref, b_gate_ref, ln_out_ref,
           w_out_ref, b_out_ref, out_ref, ab_send, ab_recv, o_send, o_recv, stage_a, stage_b, turned, zt, znt, gate,
           wp, bp, wg, wo, vec, keep, sides_sent, sides_here, sums_sent, sums_here):
    rows, cols, channels = z_ref.shape
    tiles = cols // LANES
    group = 4
    order = send_order(side)
    me = lax.axis_index("dap")
    core, place = lax.rem(me, 2), me // 2
    my_x, my_y = lax.rem(place, side), place // side
    my_rows = pl.ds(pl.multiple_of(me * rows, rows), rows)

    barrier = pltpu.get_barrier_semaphore()
    for step in range(1, n):
        pl.semaphore_signal(barrier, inc=1, device_id={"dap": lax.rem(me + step, n)}, device_id_type=MESH)

    def lanes(t):
        return pl.ds(pl.multiple_of(t * LANES, LANES), LANES)

    def loop(count, body):
        def step(index, carry):
            body(index)
            return carry

        lax.fori_loop(0, count, step, 0)

    def send_all(source_of, target, send_sem, recv_sem):
        for dy, dx, dc in order:
            y, x, c = lax.rem(my_y + dy, side), lax.rem(my_x + dx, side), lax.rem(core + dc, 2)
            peer = (y * side + x) * 2 + c
            pltpu.make_async_remote_copy(source_of(peer), target, send_sem, recv_sem,
                                         device_id={"dap": peer}, device_id_type=MESH).start()
        pltpu.make_async_copy(source_of(me), target, recv_sem).start()

    def wait_bytes(ref, sem):
        pltpu.make_async_copy(ref, ref, sem).wait()

    def send_sides(layer, slot, t):
        send_all(lambda peer: ab_send.at[slot, peer, :, :, lanes(t)], ab_recv.at[layer, slot, :, my_rows, lanes(t)],
                 sides_sent.at[layer, slot], sides_here.at[layer, slot])

    def wait_sides(layer, slot):
        wait_bytes(ab_recv.at[layer, slot], sides_here.at[layer, slot])

    def wait_sides_sent(layer, slot):
        wait_bytes(ab_send.at[slot, pl.ds(0, n - 1)], sides_sent.at[layer, slot])

    def send_sums(layer, slot, t):
        send_all(lambda peer: o_send.at[t, slot, pl.ds(pl.multiple_of(peer * rows, rows), rows), :],
                 o_recv.at[t, pl.ds(pl.multiple_of((slot * n + me) * pitch, 8), rows), :],
                 sums_sent.at[layer, t], sums_here.at[layer, t])

    def wait_sums(layer, t):
        wait_bytes(o_send.at[t], sums_here.at[layer, t])

    def wait_sums_sent(layer, t):
        wait_bytes(o_send.at[t, :, pl.ds(0, (n - 1) * rows), :], sums_sent.at[layer, t])

    def column(row):
        return jnp.broadcast_to(row.astype(F32), (LANES, row.shape[-1])).T

    def prepare_first(layer):
        for block in range(4):
            part = slice(block * channels, (block + 1) * channels)
            weight = w_proj_ref[layer, :, part].astype(F32).T.astype(BF16)
            bias = column(b_proj_ref[layer:layer + 1, part])
            for slot in range(slots):
                wp[layer, slot, block * n:(block + 1) * n] = weight[slot * n:(slot + 1) * n]
                bp[layer, slot, block * n:(block + 1) * n] = bias[slot * n:(slot + 1) * n]
        vec[layer, 0] = column(ln_in_ref[layer, 0:1])
        vec[layer, 1] = column(ln_in_ref[layer, 1:2])

    def prepare_rest(layer):
        wg[layer] = w_gate_ref[layer].astype(F32).T.astype(BF16)
        wo[layer] = w_out_ref[layer].astype(F32).T.astype(BF16)
        vec[layer, 2] = column(b_gate_ref[layer:layer + 1])
        vec[layer, 3] = column(ln_out_ref[layer, 0:1])
        vec[layer, 4] = column(ln_out_ref[layer, 1:2])
        vec[layer, 5] = column(b_out_ref[layer:layer + 1])

    def first_norm(t):
        def some(step):
            for k in range(group):
                i = step * group + k
                values = z_ref[i, lanes(t), :].astype(F32).T
                zt[i, :, lanes(t)] = values.astype(BF16)
                znt[i, :, lanes(t)] = norm_rows(values, vec[0, 0], vec[0, 1])

        loop(rows // group, some)

    def gated(layer, slot, pairs):
        normed = jnp.concatenate([znt[i, :, lanes(t)] for i, t in pairs], axis=1)
        projected = dot(wp[layer, slot], normed, ((1,), (0,)))
        bias = bp[layer, slot]
        for k, (i, t) in enumerate(pairs):
            part = projected[:, k * LANES:(k + 1) * LANES] + bias
            kept = keep[t, pl.ds(i, 1), :]
            stage_a[t, pl.ds(i, n, stride=pitch), :] = kept * jax.nn.sigmoid(part[n:2 * n]) * part[:n]
            stage_b[t, pl.ds(i, n, stride=pitch), :] = kept * jax.nn.sigmoid(part[3 * n:]) * part[2 * n:3 * n]

    def pack(slot, tile_list, unroll):
        def some(step):
            for k in range(unroll):
                d = step * unroll + k
                start = pl.multiple_of(d * pitch, 8)
                for t in tile_list:
                    ab_send[slot, d, 0, :, lanes(t)] = stage_a[t, pl.ds(start, rows), :].astype(BF16)
                    ab_send[slot, d, 1, :, lanes(t)] = stage_b[t, pl.ds(start, rows), :].astype(BF16)

        loop(n // unroll, some)

    def make_sides(layer, slot):
        loop(rows, lambda i: gated(layer, slot, [(i, t) for t in range(tiles)]))
        pack(slot, range(tiles), 1)

    def make_sides_part(layer, t):
        loop(rows // group, lambda step: gated(layer, 0, [(step * group + k, t) for k in range(group)]))
        pack(0, [t], 4)

    def make_gates(layer):
        def row(i):
            projected = dot(wg[layer], znt[i], ((1,), (0,)))
            for t in range(tiles):
                part = slice(t * LANES, (t + 1) * LANES)
                gate[i, :, part] = jax.nn.sigmoid(projected[:, part] + vec[layer, 2])

        loop(rows, row)

    def turn(layer, slot):
        if layer == 1:
            turned[...] = ab_recv[1, slot, 0].T

    def triangle(layer, slot, t):
        if layer == 0:
            o_send[t, slot] = dot(ab_recv[0, slot, 0], ab_recv[0, slot, 1, lanes(t), :], ((1,), (1,)))
        else:
            o_send[t, slot] = dot(turned[...], ab_recv[1, slot, 1, :, lanes(t)], ((1,), (0,)))

    def finish(layer, t):
        def some(step):
            places = [step * group + k for k in range(group)]
            normed = [norm_rows(o_recv[t, pl.ds(i, channels, stride=pitch), :], vec[layer, 3], vec[layer, 4]) for i in places]
            update = dot(wo[layer], jnp.concatenate(normed, axis=1), ((1,), (0,)))
            for k, i in enumerate(places):
                added = update[:, k * LANES:(k + 1) * LANES] + vec[layer, 5]
                new = (zt[i, :, lanes(t)].astype(F32) + gate[i, :, lanes(t)] * added).astype(BF16)
                if layer == 0:
                    zt[i, :, lanes(t)] = new
                    znt[i, :, lanes(t)] = norm_rows(new.astype(F32), vec[1, 0], vec[1, 1])
                else:
                    out_ref[i, :, lanes(t)] = new

        loop(rows // group, some)

    prepare_first(0)
    for t in range(tiles):
        keep[t] = mask_ref[:, t * LANES:(t + 1) * LANES].astype(F32)

    def start(t):
        first_norm(t)
        make_sides_part(0, t)

        @pl.when(t == 0)
        def _():
            pl.semaphore_wait(barrier, n - 1)

        send_sides(0, 0, t)

    loop(tiles, start)
    for layer in range(2):
        def give_sides(step):
            if layer == 1:
                wait_sides_sent(0, step + 1)
            make_sides(layer, step + 1)
            loop(tiles, lambda t: send_sides(layer, step + 1, t))

        def give_sums(slot):
            wait_sides(layer, slot)
            turn(layer, slot)

            def some(t):
                triangle(layer, slot, t)
                send_sums(layer, slot, t)

            loop(tiles, some)

        def take_sums(t):
            wait_sums(layer, t)
            finish(layer, t)
            if layer == 0:
                make_sides_part(1, t)
                send_sides(1, 0, t)

        loop(slots - 1, give_sides)
        if layer == 0:
            prepare_rest(0)
            prepare_first(1)
            prepare_rest(1)
        make_gates(layer)
        if layer == 1:
            loop(tiles, lambda t: wait_sums_sent(0, t))
        loop(slots, give_sums)
        if layer == 0:
            wait_sides_sent(0, 0)
        loop(tiles, take_sums)

    loop(slots, lambda slot: wait_sides_sent(1, slot))
    loop(tiles, lambda t: wait_sums_sent(1, t))


def solution(mesh):
    n = mesh.shape["dap"]
    side = math.isqrt(n // 2)
    row_spec = P(("batch", "dap"), None, None)
    mask_spec = P(("batch", "dap"), None)

    def local_layers(pair, *others):
        rows, cols, channels = pair.shape
        slots = channels // n
        tiles = cols // LANES
        pitch = rows + 8
        vmem = pl.BlockSpec(memory_space=pltpu.VMEM)
        turned_out = pl.pallas_call(
            functools.partial(kernel, n, side, slots, pitch),
            out_shape=jax.ShapeDtypeStruct((rows, channels, cols), BF16),
            in_specs=[vmem] * (1 + len(others)),
            out_specs=vmem,
            scratch_shapes=[
                pltpu.VMEM((slots, n, 2, rows, cols), BF16),
                pltpu.VMEM((2, slots, 2, cols, cols), BF16),
                pltpu.VMEM((tiles, slots, cols, LANES), F32),
                pltpu.VMEM((tiles, channels * pitch, LANES), F32),
                pltpu.VMEM((tiles, n * pitch, LANES), F32),
                pltpu.VMEM((tiles, n * pitch, LANES), F32),
                pltpu.VMEM((cols, cols), BF16),
                pltpu.VMEM((rows, channels, cols), BF16),
                pltpu.VMEM((rows, channels, cols), BF16),
                pltpu.VMEM((rows, channels, cols), F32),
                pltpu.VMEM((2, slots, 4 * n, channels), BF16),
                pltpu.VMEM((2, slots, 4 * n, LANES), F32),
                pltpu.VMEM((2, channels, channels), BF16),
                pltpu.VMEM((2, channels, channels), BF16),
                pltpu.VMEM((2, 6, channels, LANES), F32),
                pltpu.VMEM((tiles, rows, LANES), F32),
                pltpu.SemaphoreType.DMA((2, slots)),
                pltpu.SemaphoreType.DMA((2, slots)),
                pltpu.SemaphoreType.DMA((2, tiles)),
                pltpu.SemaphoreType.DMA((2, tiles)),
            ],
            compiler_params=pltpu.CompilerParams(collective_id=0, has_side_effects=True, vmem_limit_bytes=60 * 2 ** 20),
            name="triangle_pair",
        )(pair, *others)
        return jnp.swapaxes(turned_out, 1, 2)

    return jax.shard_map(local_layers, mesh=mesh,
                         in_specs=(row_spec, mask_spec, P(), P(), P(), P(), P(), P(), P(), P()),
                         out_specs=row_spec, check_vma=False)
```

```python
import functools
import math

import jax
import jax.numpy as jnp
from jax import lax
from jax.experimental import pallas as pl
from jax.experimental.pallas import tpu as pltpu
from jax.sharding import PartitionSpec as P

LN_EPS = 1e-5
LANES = 128
MESH = pl.DeviceIdType.MESH
F32 = jnp.float32
BF16 = jnp.bfloat16


def send_order(side):
    near = [(1, 0), (-1, 0), (0, 1), (0, -1), (2, 0), (0, 2), (1, 1), (-1, -1), (1, -1), (-1, 1), (2, 2), (1, 2),
            (-1, 2), (2, 1), (2, -1), (0, 0)]
    found, order = set(), []
    for dc in range(2):
        for dx, dy in near + [(x, y) for x in range(side) for y in range(side)]:
            offset = (dy % side, dx % side, dc)
            if offset not in found and offset != (0, 0, 0):
                found.add(offset)
                order.append(offset)
    return order


def dot(left, right, dims):
    return lax.dot_general(left, right, (dims, ((), ())), preferred_element_type=F32)


def norm_rows(values, scale, offset):
    count = values.shape[0]
    centred = values - jnp.sum(values, axis=0, keepdims=True) * (1.0 / count)
    variance = jnp.sum(centred * centred, axis=0, keepdims=True) * (1.0 / count)
    return (centred * lax.rsqrt(variance + LN_EPS) * scale + offset).astype(BF16)


def kernel(n, side, slots, pitch, z_hbm, mask_hbm, ln_in_hbm, w_proj_hbm, b_proj_hbm, w_gate_hbm, b_gate_hbm, ln_out_hbm,
           w_out_hbm, b_out_hbm, out_ref, z_ref, mask_ref, ln_in_ref, w_proj_ref, b_proj_ref, w_gate_ref, b_gate_ref, ln_out_ref,
           w_out_ref, b_out_ref, z_here, weight_here, ab_send, ab_recv, o_send, o_recv, stage_a, stage_b, turned, zt, znt, gate,
           wp, bp, wg, wo, vec, keep, sides_sent, sides_here, sums_sent, sums_here):
    rows, cols, channels = z_ref.shape
    tiles = cols // LANES
    group = 4
    order = send_order(side)
    me = lax.axis_index("dap")
    core, place = lax.rem(me, 2), me // 2
    my_x, my_y = lax.rem(place, side), place // side
    my_rows = pl.ds(pl.multiple_of(me * rows, rows), rows)

    first_weights = [(w_proj_hbm, w_proj_ref), (b_proj_hbm, b_proj_ref), (ln_in_hbm, ln_in_ref), (mask_hbm, mask_ref)]
    rest_weights = [(w_gate_hbm, w_gate_ref), (b_gate_hbm, b_gate_ref), (ln_out_hbm, ln_out_ref), (w_out_hbm, w_out_ref),
                    (b_out_hbm, b_out_ref)]
    first_copies, rest_copies = [
        [pltpu.make_async_copy(source, target, weight_here.at[base + k]) for k, (source, target) in enumerate(group_refs)]
        for base, group_refs in ((0, first_weights), (len(first_weights), rest_weights))]

    def z_copy(t):
        part = pl.ds(pl.multiple_of(t * LANES, LANES), LANES)
        return pltpu.make_async_copy(z_hbm.at[:, part, :], z_ref.at[:, part, :], z_here.at[t])

    for copy in first_copies:
        copy.start()
    for t in range(tiles):
        z_copy(t).start()
    for copy in rest_copies:
        copy.start()

    barrier = pltpu.get_barrier_semaphore()
    for step in range(1, n):
        pl.semaphore_signal(barrier, inc=1, device_id={"dap": lax.rem(me + step, n)}, device_id_type=MESH)

    def lanes(t):
        return pl.ds(pl.multiple_of(t * LANES, LANES), LANES)

    def loop(count, body):
        def step(index, carry):
            body(index)
            return carry

        lax.fori_loop(0, count, step, 0)

    def send_all(source_of, target, send_sem, recv_sem):
        for dy, dx, dc in order:
            y, x, c = lax.rem(my_y + dy, side), lax.rem(my_x + dx, side), lax.rem(core + dc, 2)
            peer = (y * side + x) * 2 + c
            pltpu.make_async_remote_copy(source_of(peer), target, send_sem, recv_sem,
                                         device_id={"dap": peer}, device_id_type=MESH).start()
        pltpu.make_async_copy(source_of(me), target, recv_sem).start()

    def wait_bytes(ref, sem):
        pltpu.make_async_copy(ref, ref, sem).wait()

    def send_sides(layer, slot, t):
        send_all(lambda peer: ab_send.at[slot, peer, :, :, lanes(t)], ab_recv.at[layer, slot, :, my_rows, lanes(t)],
                 sides_sent.at[layer, slot], sides_here.at[layer, slot])

    def wait_sides(layer, slot):
        wait_bytes(ab_recv.at[layer, slot], sides_here.at[layer, slot])

    def wait_sides_sent(layer, slot):
        wait_bytes(ab_send.at[slot, pl.ds(0, n - 1)], sides_sent.at[layer, slot])

    def send_sums(layer, slot, t):
        send_all(lambda peer: o_send.at[t, slot, pl.ds(pl.multiple_of(peer * rows, rows), rows), :],
                 o_recv.at[t, pl.ds(pl.multiple_of((slot * n + me) * pitch, 8), rows), :],
                 sums_sent.at[layer, t], sums_here.at[layer, t])

    def wait_sums(layer, t):
        wait_bytes(o_send.at[t], sums_here.at[layer, t])

    def wait_sums_sent(layer, t):
        wait_bytes(o_send.at[t, :, pl.ds(0, (n - 1) * rows), :], sums_sent.at[layer, t])

    def column(row):
        return jnp.broadcast_to(row.astype(F32), (LANES, row.shape[-1])).T

    def prepare_first(layer):
        for block in range(4):
            part = slice(block * channels, (block + 1) * channels)
            weight = w_proj_ref[layer, :, part].astype(F32).T.astype(BF16)
            bias = column(b_proj_ref[layer:layer + 1, part])
            for slot in range(slots):
                wp[layer, slot, block * n:(block + 1) * n] = weight[slot * n:(slot + 1) * n]
                bp[layer, slot, block * n:(block + 1) * n] = bias[slot * n:(slot + 1) * n]
        vec[layer, 0] = column(ln_in_ref[layer, 0:1])
        vec[layer, 1] = column(ln_in_ref[layer, 1:2])

    def prepare_rest(layer):
        wg[layer] = w_gate_ref[layer].astype(F32).T.astype(BF16)
        wo[layer] = w_out_ref[layer].astype(F32).T.astype(BF16)
        vec[layer, 2] = column(b_gate_ref[layer:layer + 1])
        vec[layer, 3] = column(ln_out_ref[layer, 0:1])
        vec[layer, 4] = column(ln_out_ref[layer, 1:2])
        vec[layer, 5] = column(b_out_ref[layer:layer + 1])

    def first_norm(t):
        def some(step):
            for k in range(group):
                i = step * group + k
                values = z_ref[i, lanes(t), :].astype(F32).T
                zt[i, :, lanes(t)] = values.astype(BF16)
                znt[i, :, lanes(t)] = norm_rows(values, vec[0, 0], vec[0, 1])

        loop(rows // group, some)

    def gated(layer, slot, pairs):
        normed = jnp.concatenate([znt[i, :, lanes(t)] for i, t in pairs], axis=1)
        projected = dot(wp[layer, slot], normed, ((1,), (0,)))
        bias = bp[layer, slot]
        for k, (i, t) in enumerate(pairs):
            part = projected[:, k * LANES:(k + 1) * LANES] + bias
            kept = keep[t, pl.ds(i, 1), :]
            stage_a[t, pl.ds(i, n, stride=pitch), :] = kept * jax.nn.sigmoid(part[n:2 * n]) * part[:n]
            stage_b[t, pl.ds(i, n, stride=pitch), :] = kept * jax.nn.sigmoid(part[3 * n:]) * part[2 * n:3 * n]

    def pack(slot, tile_list, unroll):
        def some(step):
            for k in range(unroll):
                d = step * unroll + k
                start = pl.multiple_of(d * pitch, 8)
                for t in tile_list:
                    ab_send[slot, d, 0, :, lanes(t)] = stage_a[t, pl.ds(start, rows), :].astype(BF16)
                    ab_send[slot, d, 1, :, lanes(t)] = stage_b[t, pl.ds(start, rows), :].astype(BF16)

        loop(n // unroll, some)

    def make_sides(layer, slot):
        loop(rows, lambda i: gated(layer, slot, [(i, t) for t in range(tiles)]))
        pack(slot, range(tiles), 1)

    def make_sides_part(layer, t):
        loop(rows // group, lambda step: gated(layer, 0, [(step * group + k, t) for k in range(group)]))
        pack(0, [t], 4)

    def make_gates(layer):
        def row(i):
            projected = dot(wg[layer], znt[i], ((1,), (0,)))
            for t in range(tiles):
                part = slice(t * LANES, (t + 1) * LANES)
                gate[i, :, part] = jax.nn.sigmoid(projected[:, part] + vec[layer, 2])

        loop(rows, row)

    def turn(layer, slot):
        if layer == 1:
            turned[...] = ab_recv[1, slot, 0].T

    def triangle(layer, slot, t):
        if layer == 0:
            o_send[t, slot] = dot(ab_recv[0, slot, 0], ab_recv[0, slot, 1, lanes(t), :], ((1,), (1,)))
        else:
            o_send[t, slot] = dot(turned[...], ab_recv[1, slot, 1, :, lanes(t)], ((1,), (0,)))

    def finish(layer, t):
        def some(step):
            places = [step * group + k for k in range(group)]
            normed = [norm_rows(o_recv[t, pl.ds(i, channels, stride=pitch), :], vec[layer, 3], vec[layer, 4]) for i in places]
            update = dot(wo[layer], jnp.concatenate(normed, axis=1), ((1,), (0,)))
            for k, i in enumerate(places):
                added = update[:, k * LANES:(k + 1) * LANES] + vec[layer, 5]
                new = (zt[i, :, lanes(t)].astype(F32) + gate[i, :, lanes(t)] * added).astype(BF16)
                if layer == 0:
                    zt[i, :, lanes(t)] = new
                    znt[i, :, lanes(t)] = norm_rows(new.astype(F32), vec[1, 0], vec[1, 1])
                else:
                    out_ref[i, lanes(t), :] = new.astype(F32).T.astype(BF16)

        loop(rows // group, some)

    for copy in first_copies:
        copy.wait()
    prepare_first(0)
    for t in range(tiles):
        keep[t] = mask_ref[:, t * LANES:(t + 1) * LANES].astype(F32)

    def start(t):
        z_copy(t).wait()
        first_norm(t)
        make_sides_part(0, t)

        @pl.when(t == 0)
        def _():
            pl.semaphore_wait(barrier, n - 1)

        send_sides(0, 0, t)

    loop(tiles, start)
    for layer in range(2):
        def give_sides(step):
            if layer == 1:
                wait_sides_sent(0, step + 1)
            make_sides(layer, step + 1)
            loop(tiles, lambda t: send_sides(layer, step + 1, t))

        def give_sums(slot):
            wait_sides(layer, slot)
            turn(layer, slot)

            def some(t):
                triangle(layer, slot, t)
                send_sums(layer, slot, t)

            loop(tiles, some)

        def take_sums(t):
            wait_sums(layer, t)
            finish(layer, t)
            if layer == 0:
                make_sides_part(1, t)
                send_sides(1, 0, t)

        loop(slots - 1, give_sides)
        if layer == 0:
            for copy in rest_copies:
                copy.wait()
            prepare_rest(0)
            prepare_first(1)
            prepare_rest(1)
        make_gates(layer)
        if layer == 1:
            loop(tiles, lambda t: wait_sums_sent(0, t))
        loop(slots, give_sums)
        if layer == 0:
            wait_sides_sent(0, 0)
        loop(tiles, take_sums)

    loop(slots, lambda slot: wait_sides_sent(1, slot))
    loop(tiles, lambda t: wait_sums_sent(1, t))


def solution(mesh):
    n = mesh.shape["dap"]
    side = math.isqrt(n // 2)
    row_spec = P(("batch", "dap"), None, None)
    mask_spec = P(("batch", "dap"), None)

    def local_layers(pair, *others):
        rows, cols, channels = pair.shape
        slots = channels // n
        tiles = cols // LANES
        pitch = rows + 8
        operands = (pair,) + others
        return pl.pallas_call(
            functools.partial(kernel, n, side, slots, pitch),
            out_shape=pltpu.VMEM(pair.shape, BF16),
            in_specs=[pl.BlockSpec(memory_space=pltpu.HBM)] * len(operands),
            out_specs=pl.BlockSpec(memory_space=pltpu.VMEM),
            scratch_shapes=[pltpu.VMEM(operand.shape, operand.dtype) for operand in operands] + [
                pltpu.SemaphoreType.DMA((tiles,)),
                pltpu.SemaphoreType.DMA((len(operands) - 1,)),
                pltpu.VMEM((slots, n, 2, rows, cols), BF16),
                pltpu.VMEM((2, slots, 2, cols, cols), BF16),
                pltpu.VMEM((tiles, slots, cols, LANES), F32),
                pltpu.VMEM((tiles, channels * pitch, LANES), F32),
                pltpu.VMEM((tiles, n * pitch, LANES), F32),
                pltpu.VMEM((tiles, n * pitch, LANES), F32),
                pltpu.VMEM((cols, cols), BF16),
                pltpu.VMEM((rows, channels, cols), BF16),
                pltpu.VMEM((rows, channels, cols), BF16),
                pltpu.VMEM((rows, channels, cols), F32),
                pltpu.VMEM((2, slots, 4 * n, channels), BF16),
                pltpu.VMEM((2, slots, 4 * n, LANES), F32),
                pltpu.VMEM((2, channels, channels), BF16),
                pltpu.VMEM((2, channels, channels), BF16),
                pltpu.VMEM((2, 6, channels, LANES), F32),
                pltpu.VMEM((tiles, rows, LANES), F32),
                pltpu.SemaphoreType.DMA((2, slots)),
                pltpu.SemaphoreType.DMA((2, slots)),
                pltpu.SemaphoreType.DMA((2, tiles)),
                pltpu.SemaphoreType.DMA((2, tiles)),
            ],
            compiler_params=pltpu.CompilerParams(collective_id=0, has_side_effects=True, vmem_limit_bytes=54 * 2 ** 20),
            name="triangle_pair",
        )(*operands)

    return jax.shard_map(local_layers, mesh=mesh,
                         in_specs=(row_spec, mask_spec, P(), P(), P(), P(), P(), P(), P(), P()),
                         out_specs=row_spec, check_vma=False)
```

```python
import functools
import math

import jax
import jax.numpy as jnp
from jax import lax
from jax.experimental import pallas as pl
from jax.experimental.pallas import tpu as pltpu
from jax.sharding import PartitionSpec as P

LN_EPS = 1e-5
LANES = 128
MESH = pl.DeviceIdType.MESH
F32 = jnp.float32
BF16 = jnp.bfloat16


def send_order(side):
    near = [(1, 0), (-1, 0), (0, 1), (0, -1), (2, 0), (0, 2), (1, 1), (-1, -1), (1, -1), (-1, 1), (2, 2), (1, 2),
            (-1, 2), (2, 1), (2, -1), (0, 0)]
    found, order = set(), []
    for dc in range(2):
        for dx, dy in near + [(x, y) for x in range(side) for y in range(side)]:
            offset = (dy % side, dx % side, dc)
            if offset not in found and offset != (0, 0, 0):
                found.add(offset)
                order.append(offset)
    return order


def group_order(side):
    ring = [step % side for step in (1, -1)] + [0] + [step % side for step in (1, -1)] + [2 % side, 2 % side, 0]
    flips = [0, 0, 1, 1, 1, 0, 1, 0]
    return [(unit, step, flip, dc) for dc in range(2) for step, flip in zip(ring, flips) for unit in range(2)
            if (step, flip, dc) != (0, 0, 0)]


def dot(left, right, dims):
    return lax.dot_general(left, right, (dims, ((), ())), preferred_element_type=F32)


def norm_rows(values, scale, offset):
    count = values.shape[0]
    centred = values - jnp.sum(values, axis=0, keepdims=True) * (1.0 / count)
    variance = jnp.sum(centred * centred, axis=0, keepdims=True) * (1.0 / count)
    return (centred * lax.rsqrt(variance + LN_EPS) * scale + offset).astype(BF16)


def kernel(n, side, slots, pitch, z_hbm, mask_hbm, ln_in_hbm, w_proj_hbm, b_proj_hbm, w_gate_hbm, b_gate_hbm, ln_out_hbm,
           w_out_hbm, b_out_hbm, out_ref, z_ref, mask_ref, ln_in_ref, w_proj_ref, b_proj_ref, w_gate_ref, b_gate_ref, ln_out_ref,
           w_out_ref, b_out_ref, z_here, weight_here, ab_send, a_first, b_first, ab_recv, o_send, o_recv, stage_a, stage_b, turned, zt, znt, gate,
           wp, bp, wg, wo, vec, keep, sides_sent, sides_here, sums_sent, sums_here, twin_sent, twin_here):
    rows, cols, channels = z_ref.shape
    tiles = cols // LANES
    group = 4
    order = send_order(side)
    me = lax.axis_index("dap")
    core, place = lax.rem(me, 2), me // 2
    my_x, my_y = lax.rem(place, side), place // side
    my_rows = pl.ds(pl.multiple_of(me * rows, rows), rows)

    first_weights = [(w_proj_hbm, w_proj_ref), (b_proj_hbm, b_proj_ref), (ln_in_hbm, ln_in_ref), (mask_hbm, mask_ref)]
    rest_weights = [(w_gate_hbm, w_gate_ref), (b_gate_hbm, b_gate_ref), (ln_out_hbm, ln_out_ref), (w_out_hbm, w_out_ref),
                    (b_out_hbm, b_out_ref)]
    first_copies, rest_copies = [
        [pltpu.make_async_copy(source, target, weight_here.at[base + k]) for k, (source, target) in enumerate(group_refs)]
        for base, group_refs in ((0, first_weights), (len(first_weights), rest_weights))]

    def z_copy(t):
        part = pl.ds(pl.multiple_of(t * LANES, LANES), LANES)
        return pltpu.make_async_copy(z_hbm.at[:, part, :], z_ref.at[:, part, :], z_here.at[t])

    for copy in first_copies:
        copy.start()
    for t in range(tiles):
        z_copy(t).start()
    for copy in rest_copies:
        copy.start()

    barrier = pltpu.get_barrier_semaphore()
    for step in range(1, n):
        pl.semaphore_signal(barrier, inc=1, device_id={"dap": lax.rem(me + step, n)}, device_id_type=MESH)

    def lanes(t):
        return pl.ds(pl.multiple_of(t * LANES, LANES), LANES)

    def loop(count, body):
        def step(index, carry):
            body(index)
            return carry

        lax.fori_loop(0, count, step, 0)

    def send_all(source_of, target, send_sem, recv_sem):
        for dy, dx, dc in order:
            y, x, c = lax.rem(my_y + dy, side), lax.rem(my_x + dx, side), lax.rem(core + dc, 2)
            peer = (y * side + x) * 2 + c
            pltpu.make_async_remote_copy(source_of(peer), target, send_sem, recv_sem,
                                         device_id={"dap": peer}, device_id_type=MESH).start()
        pltpu.make_async_copy(source_of(me), target, recv_sem).start()

    def wait_bytes(ref, sem):
        pltpu.make_async_copy(ref, ref, sem).wait()

    half = n // 2

    def place_of(unit, slot):
        along, across = (my_y, my_x) if unit == 0 else (my_x, my_y)
        shift = lax.rem(slot, 2)
        turned_along = lax.rem(along + shift, side)
        return shift, turned_along, turned_along // 2, across

    def entry(unit, turned_along, pair, across, c):
        return unit * half + (lax.rem(turned_along + pair, 2) * side + across) * 2 + c

    def device(unit, turned_along, shift, across, c):
        along = lax.rem(turned_along + side - shift, side)
        return ((along * side + across) if unit == 0 else (across * side + along)) * 2 + c

    def my_entries(slot):
        entries = []
        for unit in range(2):
            shift, turned_along, pair, across = place_of(unit, slot)
            entries.append(entry(unit, turned_along, pair, across, core))
        return entries

    def group_peers(couple):
        for unit, step, flip, dc in group_order(side):
            for slot in couple:
                shift, turned_along, pair, across = place_of(unit, slot)
                there = turned_along + (1 - 2 * (turned_along - 2 * pair)) if flip else turned_along
                across_there, c = lax.rem(across + step, side), lax.rem(core + dc, 2)
                yield slot, unit, entry(unit, there, pair, across_there, c), device(unit, there, shift, across_there, c)

    def couple_of(step):
        return 2 * step, 2 * step + 1

    def entry_rows(index):
        return pl.ds(pl.multiple_of(index * rows, rows), rows)

    def send_first_sides(step, t, width):
        part = pl.ds(pl.multiple_of(t * LANES, LANES), width)
        couple = couple_of(step)

        def copies(slot, unit, index, mine):
            return ((ab_send.at[slot, index, 0, :, part], a_first.at[slot, entry_rows(mine), part]),
                    (ab_send.at[slot, index, 1, :, part], b_first.at[slot, unit, my_rows, part]))

        entries = [my_entries(slot) for slot in couple]
        for count, (slot, unit, index, peer) in enumerate(group_peers(couple)):
            for source, target in copies(slot, unit, index, entries[count % 2][unit]):
                pltpu.make_async_remote_copy(source, target, sides_sent.at[0, slot], sides_here.at[0, slot],
                                             device_id={"dap": peer}, device_id_type=MESH).start()
        for slot, mine in zip(couple, entries):
            for unit in range(2):
                for source, target in copies(slot, unit, mine[unit], mine[unit]):
                    pltpu.make_async_copy(source, target, sides_here.at[0, slot]).start()

    def wait_first_sides(slot):
        wait_bytes(b_first.at[slot], sides_here.at[0, slot])

    def send_to_twin(step):
        for other in range(side):
            for k in range(2):
                for unit in range(2):
                    for slot in couple_of(step):
                        shift, turned_along, pair, across = place_of(unit, slot)
                        twin = device(unit, side - 1 - turned_along, shift, across, core)
                        chip = device(unit, 2 * pair + k, shift, other, 0)
                        block = pl.ds(pl.multiple_of(chip * rows, 2 * rows), 2 * rows)
                        pltpu.make_async_remote_copy(b_first.at[slot, unit, block, :], b_first.at[slot, unit, block, :],
                                                     twin_sent.at[slot], twin_here.at[slot],
                                                     device_id={"dap": twin}, device_id_type=MESH).start()

    def wait_twin(slot, sem):
        wait_bytes(a_first.at[slot], sem.at[slot])

    def send_first_sums(step, t):
        couple = couple_of(step)
        sent, here = sums_sent.at[0, t], sums_here.at[0, t]

        def ends(slot, index, mine):
            return (o_send.at[t, slot, entry_rows(index), :],
                    o_recv.at[t, pl.ds(pl.multiple_of((slot * n + mine) * pitch, 8), rows), :])

        entries = [my_entries(slot) for slot in couple]
        for count, (slot, unit, index, peer) in enumerate(group_peers(couple)):
            source, target = ends(slot, index, entries[count % 2][unit])
            pltpu.make_async_remote_copy(source, target, sent, here, device_id={"dap": peer}, device_id_type=MESH).start()
        for slot, mine in zip(couple, entries):
            for unit in range(2):
                source, target = ends(slot, mine[unit], mine[unit])
                pltpu.make_async_copy(source, target, here).start()

    def send_sides(layer, slot, t):
        send_all(lambda peer: ab_send.at[slot, peer, :, :, lanes(t)], ab_recv.at[slot, :, my_rows, lanes(t)],
                 sides_sent.at[layer, slot], sides_here.at[layer, slot])

    def wait_sides(layer, slot):
        wait_bytes(ab_recv.at[slot], sides_here.at[layer, slot])

    def wait_sides_sent(layer, slot):
        wait_bytes(ab_send.at[slot, pl.ds(0, n - 2 + layer)], sides_sent.at[layer, slot])

    def send_sums(layer, slot, t):
        send_all(lambda peer: o_send.at[t, slot, pl.ds(pl.multiple_of(peer * rows, rows), rows), :],
                 o_recv.at[t, pl.ds(pl.multiple_of((slot * n + me) * pitch, 8), rows), :],
                 sums_sent.at[layer, t], sums_here.at[layer, t])

    def wait_sums(layer, t):
        wait_bytes(o_send.at[t], sums_here.at[layer, t])

    def wait_sums_sent(layer, t):
        wait_bytes(o_send.at[t, :, pl.ds(0, (n - 2 + layer) * rows), :], sums_sent.at[layer, t])

    def column(row):
        return jnp.broadcast_to(row.astype(F32), (LANES, row.shape[-1])).T

    def prepare_first(layer):
        for block in range(4):
            part = slice(block * channels, (block + 1) * channels)
            weight = w_proj_ref[layer, :, part].astype(F32).T.astype(BF16)
            bias = column(b_proj_ref[layer:layer + 1, part])
            for slot in range(slots):
                wp[layer, slot, block * n:(block + 1) * n] = weight[slot * n:(slot + 1) * n]
                bp[layer, slot, block * n:(block + 1) * n] = bias[slot * n:(slot + 1) * n]
        vec[layer, 0] = column(ln_in_ref[layer, 0:1])
        vec[layer, 1] = column(ln_in_ref[layer, 1:2])

    def prepare_rest(layer):
        wg[layer] = w_gate_ref[layer].astype(F32).T.astype(BF16)
        wo[layer] = w_out_ref[layer].astype(F32).T.astype(BF16)
        vec[layer, 2] = column(b_gate_ref[layer:layer + 1])
        vec[layer, 3] = column(ln_out_ref[layer, 0:1])
        vec[layer, 4] = column(ln_out_ref[layer, 1:2])
        vec[layer, 5] = column(b_out_ref[layer:layer + 1])

    def first_norm(t):
        def some(step):
            for k in range(group):
                i = step * group + k
                values = z_ref[i, lanes(t), :].astype(F32).T
                zt[i, :, lanes(t)] = values.astype(BF16)
                znt[i, :, lanes(t)] = norm_rows(values, vec[0, 0], vec[0, 1])

        loop(rows // group, some)

    def gated(layer, slot, pairs):
        normed = jnp.concatenate([znt[i, :, lanes(t)] for i, t in pairs], axis=1)
        projected = dot(wp[layer, slot], normed, ((1,), (0,)))
        bias = bp[layer, slot]
        for k, (i, t) in enumerate(pairs):
            part = projected[:, k * LANES:(k + 1) * LANES] + bias
            kept = keep[t, pl.ds(i, 1), :]
            stage_a[t, pl.ds(i, n, stride=pitch), :] = kept * jax.nn.sigmoid(part[n:2 * n]) * part[:n]
            stage_b[t, pl.ds(i, n, stride=pitch), :] = kept * jax.nn.sigmoid(part[3 * n:]) * part[2 * n:3 * n]

    def pack(slot, tile_list, unroll):
        def some(step):
            for k in range(unroll):
                d = step * unroll + k
                start = pl.multiple_of(d * pitch, 8)
                for t in tile_list:
                    ab_send[slot, d, 0, :, lanes(t)] = stage_a[t, pl.ds(start, rows), :].astype(BF16)
                    ab_send[slot, d, 1, :, lanes(t)] = stage_b[t, pl.ds(start, rows), :].astype(BF16)

        loop(n // unroll, some)

    def make_sides(layer, slot):
        loop(rows, lambda i: gated(layer, slot, [(i, t) for t in range(tiles)]))
        pack(slot, range(tiles), 1)

    def make_sides_part(layer, slot, t):
        loop(rows // group, lambda step: gated(layer, slot, [(step * group + k, t) for k in range(group)]))
        pack(slot, [t], 4)

    def make_sides_half(layer, slot, t):
        loop(rows // 2, lambda step: gated(layer, slot, [(2 * step + k, t + j) for k in range(2) for j in range(2)]))
        pack(slot, [t, t + 1], 2)

    def make_gates(layer):
        def row(i):
            projected = dot(wg[layer], znt[i], ((1,), (0,)))
            for t in range(tiles):
                part = slice(t * LANES, (t + 1) * LANES)
                gate[i, :, part] = jax.nn.sigmoid(projected[:, part] + vec[layer, 2])

        loop(rows, row)

    def turn(layer, slot):
        if layer == 1:
            turned[...] = ab_recv[slot, 0].T

    def triangle(layer, slot, t):
        if layer == 0:
            for unit in range(2):
                part = slice(unit * half * rows, (unit + 1) * half * rows)
                o_send[t, slot, part] = dot(a_first[slot, part], b_first[slot, unit, lanes(t), :], ((1,), (1,)))
        else:
            o_send[t, slot] = dot(turned[...], ab_recv[slot, 1, :, lanes(t)], ((1,), (0,)))

    def finish(layer, t):
        def some(step):
            places = [step * group + k for k in range(group)]
            normed = [norm_rows(o_recv[t, pl.ds(i, channels, stride=pitch), :], vec[layer, 3], vec[layer, 4]) for i in places]
            update = dot(wo[layer], jnp.concatenate(normed, axis=1), ((1,), (0,)))
            for k, i in enumerate(places):
                added = update[:, k * LANES:(k + 1) * LANES] + vec[layer, 5]
                new = (zt[i, :, lanes(t)].astype(F32) + gate[i, :, lanes(t)] * added).astype(BF16)
                if layer == 0:
                    zt[i, :, lanes(t)] = new
                    znt[i, :, lanes(t)] = norm_rows(new.astype(F32), vec[1, 0], vec[1, 1])
                else:
                    out_ref[i, lanes(t), :] = new.astype(F32).T.astype(BF16)

        loop(rows // group, some)

    for copy in first_copies:
        copy.wait()
    prepare_first(0)
    for t in range(tiles):
        keep[t] = mask_ref[:, t * LANES:(t + 1) * LANES].astype(F32)

    def start(t):
        z_copy(t).wait()
        first_norm(t)
        make_sides_part(0, 0, t)
        make_sides_part(0, 1, t)

        @pl.when(t == 0)
        def _():
            pl.semaphore_wait(barrier, n - 1)

        send_first_sides(0, t, LANES)

    loop(tiles, start)
    for layer in range(2):
        def give_sides(step):
            wait_sides_sent(0, step + 1)
            make_sides(1, step + 1)
            loop(tiles, lambda t: send_sides(1, step + 1, t))

        def give_first_sums(step):
            for slot in couple_of(step):
                wait_twin(slot, twin_here)

            def some(t):
                for slot in couple_of(step):
                    triangle(0, slot, t)
                send_first_sums(step, t)

                @pl.when((t == tiles // 2 - 1) & (step < slots // 2 - 1))
                def _():
                    forward(step + 1)

            loop(tiles, some)

        def give_sums(slot):
            wait_sides(1, slot)
            turn(1, slot)

            def some(t):
                triangle(1, slot, t)
                send_sums(1, slot, t)

            loop(tiles, some)

        def take_sums(t):
            wait_sums(layer, t)
            finish(layer, t)
            if layer == 0:
                make_sides_part(1, 0, t)
                send_sides(1, 0, t)

        def forward(step):
            for slot in couple_of(step):
                wait_first_sides(slot)
            send_to_twin(step)

        if layer == 0:
            def give_first_sides(index):
                step, t = 1 + index // (tiles // 2), 2 * lax.rem(index, tiles // 2)
                for slot in couple_of(step):
                    make_sides_half(0, slot, t)
                send_first_sides(step, t, 2 * LANES)

                @pl.when(index == 1)
                def _():
                    forward(0)

            loop((slots // 2 - 1) * (tiles // 2), give_first_sides)
            for copy in rest_copies:
                copy.wait()
            prepare_rest(0)
            prepare_first(1)
            prepare_rest(1)
            make_gates(0)
            loop(slots // 2, give_first_sums)
            wait_sides_sent(0, 0)
        else:
            loop(slots - 1, give_sides)
            make_gates(1)
            loop(tiles, lambda t: wait_sums_sent(0, t))
            loop(slots, give_sums)
        loop(tiles, take_sums)

    loop(slots, lambda slot: wait_twin(slot, twin_sent))
    loop(slots, lambda slot: wait_sides_sent(1, slot))
    loop(tiles, lambda t: wait_sums_sent(1, t))


def solution(mesh):
    n = mesh.shape["dap"]
    side = math.isqrt(n // 2)
    row_spec = P(("batch", "dap"), None, None)
    mask_spec = P(("batch", "dap"), None)

    def local_layers(pair, *others):
        rows, cols, channels = pair.shape
        slots = channels // n
        tiles = cols // LANES
        pitch = rows + 8
        operands = (pair,) + others
        return pl.pallas_call(
            functools.partial(kernel, n, side, slots, pitch),
            out_shape=pltpu.VMEM(pair.shape, BF16),
            in_specs=[pl.BlockSpec(memory_space=pltpu.HBM)] * len(operands),
            out_specs=pl.BlockSpec(memory_space=pltpu.VMEM),
            scratch_shapes=[pltpu.VMEM(operand.shape, operand.dtype) for operand in operands] + [
                pltpu.SemaphoreType.DMA((tiles,)),
                pltpu.SemaphoreType.DMA((len(operands) - 1,)),
                pltpu.VMEM((slots, n, 2, rows, cols), BF16),
                pltpu.VMEM((slots, cols, cols), BF16),
                pltpu.VMEM((slots, 2, cols, cols), BF16),
                pltpu.VMEM((slots, 2, cols, cols), BF16),
                pltpu.VMEM((tiles, slots, cols, LANES), F32),
                pltpu.VMEM((tiles, channels * pitch, LANES), F32),
                pltpu.VMEM((tiles, n * pitch, LANES), F32),
                pltpu.VMEM((tiles, n * pitch, LANES), F32),
                pltpu.VMEM((cols, cols), BF16),
                pltpu.VMEM((rows, channels, cols), BF16),
                pltpu.VMEM((rows, channels, cols), BF16),
                pltpu.VMEM((rows, channels, cols), F32),
                pltpu.VMEM((2, slots, 4 * n, channels), BF16),
                pltpu.VMEM((2, slots, 4 * n, LANES), F32),
                pltpu.VMEM((2, channels, channels), BF16),
                pltpu.VMEM((2, channels, channels), BF16),
                pltpu.VMEM((2, 6, channels, LANES), F32),
                pltpu.VMEM((tiles, rows, LANES), F32),
                pltpu.SemaphoreType.DMA((2, slots)),
                pltpu.SemaphoreType.DMA((2, slots)),
                pltpu.SemaphoreType.DMA((2, tiles)),
                pltpu.SemaphoreType.DMA((2, tiles)),
                pltpu.SemaphoreType.DMA((slots,)),
                pltpu.SemaphoreType.DMA((slots,)),
            ],
            compiler_params=pltpu.CompilerParams(collective_id=0, has_side_effects=True, vmem_limit_bytes=54 * 2 ** 20),
            name="triangle_pair",
        )(*operands)

    return jax.shard_map(local_layers, mesh=mesh,
                         in_specs=(row_spec, mask_spec, P(), P(), P(), P(), P(), P(), P(), P()),
                         out_specs=row_spec, check_vma=False)
```

```python
import functools
import math

import jax
import jax.numpy as jnp
from jax import lax
from jax.experimental import pallas as pl
from jax.experimental.pallas import tpu as pltpu
from jax.sharding import PartitionSpec as P

LN_EPS = 1e-5
LANES = 128
MESH = pl.DeviceIdType.MESH
F32 = jnp.float32
BF16 = jnp.bfloat16


def send_order(side):
    near = [(1, 0), (-1, 0), (0, 1), (0, -1), (2, 0), (0, 2), (1, 1), (-1, -1), (1, -1), (-1, 1), (2, 2), (1, 2),
            (-1, 2), (2, 1), (2, -1), (0, 0)]
    found, order = set(), []
    for dc in range(2):
        for dx, dy in near + [(x, y) for x in range(side) for y in range(side)]:
            offset = (dy % side, dx % side, dc)
            if offset not in found and offset != (0, 0, 0):
                found.add(offset)
                order.append(offset)
    return order


def group_order(side):
    ring = [step % side for step in (1, -1)] + [0] + [step % side for step in (1, -1)] + [2 % side, 2 % side, 0]
    flips = [0, 0, 1, 1, 1, 0, 1, 0]
    return [(unit, step, flip, dc) for dc in range(2) for step, flip in zip(ring, flips) for unit in range(2)
            if (step, flip, dc) != (0, 0, 0)]


def dot(left, right, dims):
    return lax.dot_general(left, right, (dims, ((), ())), preferred_element_type=F32)


def norm_rows(values, scale, offset):
    count = values.shape[0]
    centred = values - jnp.sum(values, axis=0, keepdims=True) * (1.0 / count)
    variance = jnp.sum(centred * centred, axis=0, keepdims=True) * (1.0 / count)
    return (centred * lax.rsqrt(variance + LN_EPS) * scale + offset).astype(BF16)


def kernel(n, side, slots, pitch, z_hbm, mask_hbm, ln_in_hbm, w_proj_hbm, b_proj_hbm, w_gate_hbm, b_gate_hbm, ln_out_hbm,
           w_out_hbm, b_out_hbm, out_ref, z_ref, mask_ref, ln_in_ref, w_proj_ref, b_proj_ref, w_gate_ref, b_gate_ref, ln_out_ref,
           w_out_ref, b_out_ref, z_here, weight_here, ab_send, a_first, b_first, ab_recv, o_send, o_recv, stage_a, stage_b, turned, zt, znt, gate,
           wp, bp, wg, wo, vec, keep, sides_sent, sides_here, sums_sent, sums_here, twin_sent, twin_here):
    rows, cols, channels = z_ref.shape
    tiles = cols // LANES
    group = 16
    order = send_order(side)
    me = lax.axis_index("dap")
    core, place = lax.rem(me, 2), me // 2
    my_x, my_y = lax.rem(place, side), place // side
    my_rows = pl.ds(pl.multiple_of(me * rows, rows), rows)

    first_weights = [(w_proj_hbm, w_proj_ref), (b_proj_hbm, b_proj_ref), (ln_in_hbm, ln_in_ref), (mask_hbm, mask_ref)]
    rest_weights = [(w_gate_hbm, w_gate_ref), (b_gate_hbm, b_gate_ref), (ln_out_hbm, ln_out_ref), (w_out_hbm, w_out_ref),
                    (b_out_hbm, b_out_ref)]
    first_copies, rest_copies = [
        [pltpu.make_async_copy(source, target, weight_here.at[base + k]) for k, (source, target) in enumerate(group_refs)]
        for base, group_refs in ((0, first_weights), (len(first_weights), rest_weights))]

    def z_copy(t):
        part = pl.ds(pl.multiple_of(t * LANES, LANES), LANES)
        return pltpu.make_async_copy(z_hbm.at[:, part, :], z_ref.at[:, part, :], z_here.at[t])

    for copy in first_copies:
        copy.start()
    for t in range(tiles):
        z_copy(t).start()
    for copy in rest_copies:
        copy.start()

    barrier = pltpu.get_barrier_semaphore()
    for step in range(1, n):
        pl.semaphore_signal(barrier, inc=1, device_id={"dap": lax.rem(me + step, n)}, device_id_type=MESH)

    def lanes(t):
        return pl.ds(pl.multiple_of(t * LANES, LANES), LANES)

    def loop(count, body):
        def step(index, carry):
            body(index)
            return carry

        lax.fori_loop(0, count, step, 0)

    def send_all(source_of, target, send_sem, recv_sem):
        for dy, dx, dc in order:
            y, x, c = lax.rem(my_y + dy, side), lax.rem(my_x + dx, side), lax.rem(core + dc, 2)
            peer = (y * side + x) * 2 + c
            pltpu.make_async_remote_copy(source_of(peer), target, send_sem, recv_sem,
                                         device_id={"dap": peer}, device_id_type=MESH).start()
        pltpu.make_async_copy(source_of(me), target, recv_sem).start()

    def wait_bytes(ref, sem):
        pltpu.make_async_copy(ref, ref, sem).wait()

    half = n // 2

    def place_of(unit, slot):
        along, across = (my_y, my_x) if unit == 0 else (my_x, my_y)
        shift = lax.rem(slot, 2)
        turned_along = lax.rem(along + shift, side)
        return shift, turned_along, turned_along // 2, across

    def entry(unit, turned_along, pair, across, c):
        return unit * half + (lax.rem(turned_along + pair, 2) * side + across) * 2 + c

    def device(unit, turned_along, shift, across, c):
        along = lax.rem(turned_along + side - shift, side)
        return ((along * side + across) if unit == 0 else (across * side + along)) * 2 + c

    def my_entries(slot):
        entries = []
        for unit in range(2):
            shift, turned_along, pair, across = place_of(unit, slot)
            entries.append(entry(unit, turned_along, pair, across, core))
        return entries

    def group_peers(couple):
        for unit, step, flip, dc in group_order(side):
            for slot in couple:
                shift, turned_along, pair, across = place_of(unit, slot)
                there = turned_along + (1 - 2 * (turned_along - 2 * pair)) if flip else turned_along
                across_there, c = lax.rem(across + step, side), lax.rem(core + dc, 2)
                yield slot, unit, entry(unit, there, pair, across_there, c), device(unit, there, shift, across_there, c)

    def couple_of(step):
        return 2 * step, 2 * step + 1

    def entry_rows(index):
        return pl.ds(pl.multiple_of(index * rows, rows), rows)

    def send_first_sides(step, t, width):
        part = pl.ds(pl.multiple_of(t * LANES, LANES), width)
        couple = couple_of(step)

        def copies(slot, unit, index, mine):
            return ((ab_send.at[slot, index, 0, :, part], a_first.at[slot, entry_rows(mine), part]),
                    (ab_send.at[slot, index, 1, :, part], b_first.at[slot, unit, my_rows, part]))

        entries = [my_entries(slot) for slot in couple]
        for count, (slot, unit, index, peer) in enumerate(group_peers(couple)):
            for source, target in copies(slot, unit, index, entries[count % 2][unit]):
                pltpu.make_async_remote_copy(source, target, sides_sent.at[0, slot], sides_here.at[0, slot],
                                             device_id={"dap": peer}, device_id_type=MESH).start()
        for slot, mine in zip(couple, entries):
            for unit in range(2):
                for source, target in copies(slot, unit, mine[unit], mine[unit]):
                    pltpu.make_async_copy(source, target, sides_here.at[0, slot]).start()

    def wait_first_sides(slot):
        wait_bytes(b_first.at[slot], sides_here.at[0, slot])

    def send_to_twin(step):
        for other in range(side):
            for k in range(2):
                for unit in range(2):
                    for slot in couple_of(step):
                        shift, turned_along, pair, across = place_of(unit, slot)
                        twin = device(unit, side - 1 - turned_along, shift, across, core)
                        chip = device(unit, 2 * pair + k, shift, other, 0)
                        block = pl.ds(pl.multiple_of(chip * rows, 2 * rows), 2 * rows)
                        pltpu.make_async_remote_copy(b_first.at[slot, unit, block, :], b_first.at[slot, unit, block, :],
                                                     twin_sent.at[slot], twin_here.at[slot],
                                                     device_id={"dap": twin}, device_id_type=MESH).start()

    def wait_twin(slot, sem):
        wait_bytes(a_first.at[slot], sem.at[slot])

    def send_first_sums(step, t):
        couple = couple_of(step)
        sent, here = sums_sent.at[0, t], sums_here.at[0, t]

        def ends(slot, index, mine):
            return (o_send.at[t, slot, entry_rows(index), :],
                    o_recv.at[t, pl.ds(pl.multiple_of((slot * n + mine) * pitch, 8), rows), :])

        entries = [my_entries(slot) for slot in couple]
        for count, (slot, unit, index, peer) in enumerate(group_peers(couple)):
            source, target = ends(slot, index, entries[count % 2][unit])
            pltpu.make_async_remote_copy(source, target, sent, here, device_id={"dap": peer}, device_id_type=MESH).start()
        for slot, mine in zip(couple, entries):
            for unit in range(2):
                source, target = ends(slot, mine[unit], mine[unit])
                pltpu.make_async_copy(source, target, here).start()

    def send_sides(layer, slot, t):
        send_all(lambda peer: ab_send.at[slot, peer, :, :, lanes(t)], ab_recv.at[slot, :, my_rows, lanes(t)],
                 sides_sent.at[layer, slot], sides_here.at[layer, slot])

    def wait_sides(layer, slot):
        wait_bytes(ab_recv.at[slot], sides_here.at[layer, slot])

    def wait_sides_sent(layer, slot):
        wait_bytes(ab_send.at[slot, pl.ds(0, n - 2 + layer)], sides_sent.at[layer, slot])

    def send_sums(layer, slot, t):
        send_all(lambda peer: o_send.at[t, slot, pl.ds(pl.multiple_of(peer * rows, rows), rows), :],
                 o_recv.at[t, pl.ds(pl.multiple_of((slot * n + me) * pitch, 8), rows), :],
                 sums_sent.at[layer, t], sums_here.at[layer, t])

    def wait_sums(layer, t):
        wait_bytes(o_send.at[t], sums_here.at[layer, t])

    def wait_sums_sent(layer, t):
        wait_bytes(o_send.at[t, :, pl.ds(0, (n - 2 + layer) * rows), :], sums_sent.at[layer, t])

    def column(row):
        return jnp.broadcast_to(row.astype(F32), (LANES, row.shape[-1])).T

    def prepare_first(layer):
        for block in range(4):
            part = slice(block * channels, (block + 1) * channels)
            weight = w_proj_ref[layer, :, part].astype(F32).T.astype(BF16)
            bias = column(b_proj_ref[layer:layer + 1, part])
            for slot in range(slots):
                wp[layer, slot, block * n:(block + 1) * n] = weight[slot * n:(slot + 1) * n]
                bp[layer, slot, block * n:(block + 1) * n] = bias[slot * n:(slot + 1) * n]
        vec[layer, 0] = column(ln_in_ref[layer, 0:1])
        vec[layer, 1] = column(ln_in_ref[layer, 1:2])

    def prepare_rest(layer):
        wg[layer] = w_gate_ref[layer].astype(F32).T.astype(BF16)
        wo[layer] = w_out_ref[layer].astype(F32).T.astype(BF16)
        vec[layer, 2] = column(b_gate_ref[layer:layer + 1])
        vec[layer, 3] = column(ln_out_ref[layer, 0:1])
        vec[layer, 4] = column(ln_out_ref[layer, 1:2])
        vec[layer, 5] = column(b_out_ref[layer:layer + 1])

    def first_norm(t):
        def some(step):
            for k in range(group):
                i = step * group + k
                values = z_ref[i, lanes(t), :].astype(F32).T
                zt[i, :, lanes(t)] = values.astype(BF16)
                znt[i, :, lanes(t)] = norm_rows(values, vec[0, 0], vec[0, 1])

        loop(rows // group, some)

    def gated(layer, slot, pairs):
        normed = jnp.concatenate([znt[i, :, lanes(t)] for i, t in pairs], axis=1)
        projected = dot(wp[layer, slot], normed, ((1,), (0,)))
        bias = bp[layer, slot]
        for k, (i, t) in enumerate(pairs):
            part = projected[:, k * LANES:(k + 1) * LANES] + bias
            kept = keep[t, pl.ds(i, 1), :]
            stage_a[t, pl.ds(i, n, stride=pitch), :] = kept * jax.nn.sigmoid(part[n:2 * n]) * part[:n]
            stage_b[t, pl.ds(i, n, stride=pitch), :] = kept * jax.nn.sigmoid(part[3 * n:]) * part[2 * n:3 * n]

    def pack(slot, tile_list, unroll):
        def some(step):
            for k in range(unroll):
                d = step * unroll + k
                start = pl.multiple_of(d * pitch, 8)
                for t in tile_list:
                    ab_send[slot, d, 0, :, lanes(t)] = stage_a[t, pl.ds(start, rows), :].astype(BF16)
                    ab_send[slot, d, 1, :, lanes(t)] = stage_b[t, pl.ds(start, rows), :].astype(BF16)

        loop(n // unroll, some)

    def make_sides(layer, slot):
        loop(rows // 2, lambda step: gated(layer, slot, [(2 * step + k, t) for k in range(2) for t in range(tiles)]))
        pack(slot, range(tiles), 2)

    def make_sides_part(layer, slot, t):
        loop(rows // group, lambda step: gated(layer, slot, [(step * group + k, t) for k in range(group)]))
        pack(slot, [t], 8)

    def make_sides_half(layer, slot, t):
        loop(rows // 4, lambda step: gated(layer, slot, [(4 * step + k, t + j) for k in range(4) for j in range(2)]))
        pack(slot, [t, t + 1], 2)

    def make_gates(layer):
        def row(i):
            projected = dot(wg[layer], znt[i], ((1,), (0,)))
            for t in range(tiles):
                part = slice(t * LANES, (t + 1) * LANES)
                gate[i, :, part] = jax.nn.sigmoid(projected[:, part] + vec[layer, 2])

        loop(rows, row)

    def turn(layer, slot):
        if layer == 1:
            turned[...] = ab_recv[slot, 0].T

    def triangle(layer, slot, t):
        if layer == 0:
            for unit in range(2):
                part = slice(unit * half * rows, (unit + 1) * half * rows)
                o_send[t, slot, part] = dot(a_first[slot, part], b_first[slot, unit, lanes(t), :], ((1,), (1,)))
        else:
            o_send[t, slot] = dot(turned[...], ab_recv[slot, 1, :, lanes(t)], ((1,), (0,)))

    def finish(layer, t):
        def some(step):
            places = [step * group + k for k in range(group)]
            normed = [norm_rows(o_recv[t, pl.ds(i, channels, stride=pitch), :], vec[layer, 3], vec[layer, 4]) for i in places]
            update = dot(wo[layer], jnp.concatenate(normed, axis=1), ((1,), (0,)))
            for k, i in enumerate(places):
                added = update[:, k * LANES:(k + 1) * LANES] + vec[layer, 5]
                new = (zt[i, :, lanes(t)].astype(F32) + gate[i, :, lanes(t)] * added).astype(BF16)
                if layer == 0:
                    zt[i, :, lanes(t)] = new
                    znt[i, :, lanes(t)] = norm_rows(new.astype(F32), vec[1, 0], vec[1, 1])
                else:
                    out_ref[i, lanes(t), :] = new.astype(F32).T.astype(BF16)

        loop(rows // group, some)

    for copy in first_copies:
        copy.wait()
    prepare_first(0)
    for t in range(tiles):
        keep[t] = mask_ref[:, t * LANES:(t + 1) * LANES].astype(F32)

    def start(t):
        z_copy(t).wait()
        first_norm(t)
        make_sides_part(0, 0, t)
        make_sides_part(0, 1, t)

        @pl.when(t == 0)
        def _():
            pl.semaphore_wait(barrier, n - 1)

        send_first_sides(0, t, LANES)

    loop(tiles, start)
    for layer in range(2):
        def give_sides(step):
            wait_sides_sent(0, step + 1)
            make_sides(1, step + 1)
            loop(tiles, lambda t: send_sides(1, step + 1, t))

        def give_first_sums(step):
            for slot in couple_of(step):
                wait_twin(slot, twin_here)

            def some(t):
                for slot in couple_of(step):
                    triangle(0, slot, t)
                send_first_sums(step, t)

                @pl.when((t == tiles // 2 - 1) & (step < slots // 2 - 1))
                def _():
                    forward(step + 1)

            loop(tiles, some)

        def give_sums(slot):
            wait_sides(1, slot)
            turn(1, slot)

            def some(t):
                triangle(1, slot, t)
                send_sums(1, slot, t)

            loop(tiles, some)

        def take_sums(t):
            wait_sums(layer, t)
            finish(layer, t)
            if layer == 0:
                make_sides_part(1, 0, t)
                send_sides(1, 0, t)

        def forward(step):
            for slot in couple_of(step):
                wait_first_sides(slot)
            send_to_twin(step)

        if layer == 0:
            def give_first_sides(index):
                step, t = 1 + index // (tiles // 2), 2 * lax.rem(index, tiles // 2)
                for slot in couple_of(step):
                    make_sides_half(0, slot, t)
                send_first_sides(step, t, 2 * LANES)

                @pl.when(index == 1)
                def _():
                    forward(0)

            loop((slots // 2 - 1) * (tiles // 2), give_first_sides)
            for copy in rest_copies:
                copy.wait()
            prepare_rest(0)
            prepare_first(1)
            prepare_rest(1)
            make_gates(0)
            loop(slots // 2, give_first_sums)
            wait_sides_sent(0, 0)
        else:
            loop(slots - 1, give_sides)
            make_gates(1)
            loop(tiles, lambda t: wait_sums_sent(0, t))
            loop(slots, give_sums)
        loop(tiles, take_sums)

    loop(slots, lambda slot: wait_twin(slot, twin_sent))
    loop(slots, lambda slot: wait_sides_sent(1, slot))
    loop(tiles, lambda t: wait_sums_sent(1, t))


def solution(mesh):
    n = mesh.shape["dap"]
    side = math.isqrt(n // 2)
    row_spec = P(("batch", "dap"), None, None)
    mask_spec = P(("batch", "dap"), None)

    def local_layers(pair, *others):
        rows, cols, channels = pair.shape
        slots = channels // n
        tiles = cols // LANES
        pitch = rows + 8
        operands = (pair,) + others
        return pl.pallas_call(
            functools.partial(kernel, n, side, slots, pitch),
            out_shape=pltpu.VMEM(pair.shape, BF16),
            in_specs=[pl.BlockSpec(memory_space=pltpu.HBM)] * len(operands),
            out_specs=pl.BlockSpec(memory_space=pltpu.VMEM),
            scratch_shapes=[pltpu.VMEM(operand.shape, operand.dtype) for operand in operands] + [
                pltpu.SemaphoreType.DMA((tiles,)),
                pltpu.SemaphoreType.DMA((len(operands) - 1,)),
                pltpu.VMEM((slots, n, 2, rows, cols), BF16),
                pltpu.VMEM((slots, cols, cols), BF16),
                pltpu.VMEM((slots, 2, cols, cols), BF16),
                pltpu.VMEM((slots, 2, cols, cols), BF16),
                pltpu.VMEM((tiles, slots, cols, LANES), F32),
                pltpu.VMEM((tiles, channels * pitch, LANES), F32),
                pltpu.VMEM((tiles, n * pitch, LANES), F32),
                pltpu.VMEM((tiles, n * pitch, LANES), F32),
                pltpu.VMEM((cols, cols), BF16),
                pltpu.VMEM((rows, channels, cols), BF16),
                pltpu.VMEM((rows, channels, cols), BF16),
                pltpu.VMEM((rows, channels, cols), F32),
                pltpu.VMEM((2, slots, 4 * n, channels), BF16),
                pltpu.VMEM((2, slots, 4 * n, LANES), F32),
                pltpu.VMEM((2, channels, channels), BF16),
                pltpu.VMEM((2, channels, channels), BF16),
                pltpu.VMEM((2, 6, channels, LANES), F32),
                pltpu.VMEM((tiles, rows, LANES), F32),
                pltpu.SemaphoreType.DMA((2, slots)),
                pltpu.SemaphoreType.DMA((2, slots)),
                pltpu.SemaphoreType.DMA((2, tiles)),
                pltpu.SemaphoreType.DMA((2, tiles)),
                pltpu.SemaphoreType.DMA((slots,)),
                pltpu.SemaphoreType.DMA((slots,)),
            ],
            compiler_params=pltpu.CompilerParams(collective_id=0, has_side_effects=True, vmem_limit_bytes=54 * 2 ** 20),
            name="triangle_pair",
        )(*operands)

    return jax.shard_map(local_layers, mesh=mesh,
                         in_specs=(row_spec, mask_spec, P(), P(), P(), P(), P(), P(), P(), P()),
                         out_specs=row_spec, check_vma=False)
```

```python
import functools
import math

import jax
import jax.numpy as jnp
from jax import lax
from jax.experimental import pallas as pl
from jax.experimental.pallas import tpu as pltpu
from jax.sharding import PartitionSpec as P

LN_EPS = 1e-5
LANES = 128
MESH = pl.DeviceIdType.MESH
F32 = jnp.float32
BF16 = jnp.bfloat16


def send_order(side):
    near = [(2, 2), (1, 0), (-1, 2), (0, -1), (2, 1), (-1, 0), (1, -1), (0, 2), (1, 2), (-1, -1), (2, 0), (0, 1),
            (1, 1), (2, -1), (-1, 1), (0, 0)]
    found, order = set(), []
    for dc in range(2):
        for dx, dy in near + [(x, y) for x in range(side) for y in range(side)]:
            offset = (dy % side, dx % side, dc)
            if offset not in found and offset != (0, 0, 0):
                found.add(offset)
                order.append(offset)
    return order


def group_order(side):
    ring = [step % side for step in (1, -1)] + [0] + [step % side for step in (1, -1)] + [2 % side, 2 % side, 0]
    flips = [0, 0, 1, 1, 1, 0, 1, 0]
    return [(unit, step, flip, dc) for dc in range(2) for step, flip in zip(ring, flips) for unit in range(2)
            if (step, flip, dc) != (0, 0, 0)]


def dot(left, right, dims):
    return lax.dot_general(left, right, (dims, ((), ())), preferred_element_type=F32)


def norm_rows(values, scale, offset):
    count = values.shape[0]
    centred = values - jnp.sum(values, axis=0, keepdims=True) * (1.0 / count)
    variance = jnp.sum(centred * centred, axis=0, keepdims=True) * (1.0 / count)
    return (centred * lax.rsqrt(variance + LN_EPS) * scale + offset).astype(BF16)


def kernel(n, side, slots, pitch, z_hbm, mask_hbm, ln_in_hbm, w_proj_hbm, b_proj_hbm, w_gate_hbm, b_gate_hbm, ln_out_hbm,
           w_out_hbm, b_out_hbm, out_ref, z_ref, mask_ref, ln_in_ref, w_proj_ref, b_proj_ref, w_gate_ref, b_gate_ref, ln_out_ref,
           w_out_ref, b_out_ref, z_here, weight_here, ab_send, a_first, b_first, ab_recv, o_send, o_recv, stage_a, stage_b, turned, zt, znt, gate,
           wp, bp, wg, wo, vec, keep, sides_sent, sides_here, sums_sent, sums_here, twin_sent, twin_here):
    rows, cols, channels = z_ref.shape
    tiles = cols // LANES
    group = 16
    order = send_order(side)
    me = lax.axis_index("dap")
    core, place = lax.rem(me, 2), me // 2
    my_x, my_y = lax.rem(place, side), place // side
    my_rows = pl.ds(pl.multiple_of(me * rows, rows), rows)

    first_weights = [(w_proj_hbm, w_proj_ref), (b_proj_hbm, b_proj_ref), (ln_in_hbm, ln_in_ref), (mask_hbm, mask_ref)]
    rest_weights = [(w_gate_hbm, w_gate_ref), (b_gate_hbm, b_gate_ref), (ln_out_hbm, ln_out_ref), (w_out_hbm, w_out_ref),
                    (b_out_hbm, b_out_ref)]
    first_copies, rest_copies = [
        [pltpu.make_async_copy(source, target, weight_here.at[base + k]) for k, (source, target) in enumerate(group_refs)]
        for base, group_refs in ((0, first_weights), (len(first_weights), rest_weights))]

    def z_copy(t):
        part = pl.ds(pl.multiple_of(t * LANES, LANES), LANES)
        return pltpu.make_async_copy(z_hbm.at[:, part, :], z_ref.at[:, part, :], z_here.at[t])

    for copy in first_copies:
        copy.start()
    for t in range(tiles):
        z_copy(t).start()
    for copy in rest_copies:
        copy.start()

    barrier = pltpu.get_barrier_semaphore()
    for step in range(1, n):
        pl.semaphore_signal(barrier, inc=1, device_id={"dap": lax.rem(me + step, n)}, device_id_type=MESH)

    def lanes(t):
        return pl.ds(pl.multiple_of(t * LANES, LANES), LANES)

    def loop(count, body):
        def step(index, carry):
            body(index)
            return carry

        lax.fori_loop(0, count, step, 0)

    def send_all(source_of, target, send_sem, recv_sem):
        for dy, dx, dc in order:
            y, x, c = lax.rem(my_y + dy, side), lax.rem(my_x + dx, side), lax.rem(core + dc, 2)
            peer = (y * side + x) * 2 + c
            pltpu.make_async_remote_copy(source_of(peer), target, send_sem, recv_sem,
                                         device_id={"dap": peer}, device_id_type=MESH).start()
        pltpu.make_async_copy(source_of(me), target, recv_sem).start()

    def wait_bytes(ref, sem):
        pltpu.make_async_copy(ref, ref, sem).wait()

    half = n // 2

    def place_of(unit, slot):
        along, across = (my_y, my_x) if unit == 0 else (my_x, my_y)
        shift = lax.rem(slot, 2)
        turned_along = lax.rem(along + shift, side)
        return shift, turned_along, turned_along // 2, across

    def entry(unit, turned_along, pair, across, c):
        return unit * half + (lax.rem(turned_along + pair, 2) * side + across) * 2 + c

    def device(unit, turned_along, shift, across, c):
        along = lax.rem(turned_along + side - shift, side)
        return ((along * side + across) if unit == 0 else (across * side + along)) * 2 + c

    def my_entries(slot):
        entries = []
        for unit in range(2):
            shift, turned_along, pair, across = place_of(unit, slot)
            entries.append(entry(unit, turned_along, pair, across, core))
        return entries

    def group_peers(couple):
        for unit, step, flip, dc in group_order(side):
            for slot in couple:
                shift, turned_along, pair, across = place_of(unit, slot)
                there = turned_along + (1 - 2 * (turned_along - 2 * pair)) if flip else turned_along
                across_there, c = lax.rem(across + step, side), lax.rem(core + dc, 2)
                yield slot, unit, entry(unit, there, pair, across_there, c), device(unit, there, shift, across_there, c)

    def couple_of(step):
        return 2 * step, 2 * step + 1

    def entry_rows(index):
        return pl.ds(pl.multiple_of(index * rows, rows), rows)

    def send_first_sides(step, t, width):
        part = pl.ds(pl.multiple_of(t * LANES, LANES), width)
        couple = couple_of(step)

        def copies(slot, unit, index, mine):
            return ((ab_send.at[slot, index, 0, :, part], a_first.at[slot, entry_rows(mine), part]),
                    (ab_send.at[slot, index, 1, :, part], b_first.at[slot, unit, my_rows, part]))

        entries = [my_entries(slot) for slot in couple]
        for count, (slot, unit, index, peer) in enumerate(group_peers(couple)):
            for source, target in copies(slot, unit, index, entries[count % 2][unit]):
                pltpu.make_async_remote_copy(source, target, sides_sent.at[0, slot], sides_here.at[0, slot],
                                             device_id={"dap": peer}, device_id_type=MESH).start()
        for slot, mine in zip(couple, entries):
            for unit in range(2):
                for source, target in copies(slot, unit, mine[unit], mine[unit]):
                    pltpu.make_async_copy(source, target, sides_here.at[0, slot]).start()

    def wait_first_sides(slot):
        wait_bytes(b_first.at[slot], sides_here.at[0, slot])

    def send_to_twin(step):
        for other in range(side):
            for k in range(2):
                for unit in range(2):
                    for slot in couple_of(step):
                        shift, turned_along, pair, across = place_of(unit, slot)
                        twin = device(unit, side - 1 - turned_along, shift, across, core)
                        chip = device(unit, 2 * pair + k, shift, other, 0)
                        block = pl.ds(pl.multiple_of(chip * rows, 2 * rows), 2 * rows)
                        pltpu.make_async_remote_copy(b_first.at[slot, unit, block, :], b_first.at[slot, unit, block, :],
                                                     twin_sent.at[slot], twin_here.at[slot],
                                                     device_id={"dap": twin}, device_id_type=MESH).start()

    def wait_twin(slot, sem):
        wait_bytes(a_first.at[slot], sem.at[slot])

    def send_first_sums(step, t):
        couple = couple_of(step)
        sent, here = sums_sent.at[0, t], sums_here.at[0, t]

        def ends(slot, index, mine):
            return (o_send.at[t, slot, entry_rows(index), :],
                    o_recv.at[t, pl.ds(pl.multiple_of((slot * n + mine) * pitch, 8), rows), :])

        entries = [my_entries(slot) for slot in couple]
        for count, (slot, unit, index, peer) in enumerate(group_peers(couple)):
            source, target = ends(slot, index, entries[count % 2][unit])
            pltpu.make_async_remote_copy(source, target, sent, here, device_id={"dap": peer}, device_id_type=MESH).start()
        for slot, mine in zip(couple, entries):
            for unit in range(2):
                source, target = ends(slot, mine[unit], mine[unit])
                pltpu.make_async_copy(source, target, here).start()

    def send_sides(layer, slot, t):
        send_all(lambda peer: ab_send.at[slot, peer, :, :, lanes(t)], ab_recv.at[slot, :, my_rows, lanes(t)],
                 sides_sent.at[layer, slot], sides_here.at[layer, slot])

    def wait_sides(layer, slot):
        wait_bytes(ab_recv.at[slot], sides_here.at[layer, slot])

    def wait_sides_sent(layer, slot):
        wait_bytes(ab_send.at[slot, pl.ds(0, n - 2 + layer)], sides_sent.at[layer, slot])

    def send_sums(layer, slot, t):
        send_all(lambda peer: o_send.at[t, slot, pl.ds(pl.multiple_of(peer * rows, rows), rows), :],
                 o_recv.at[t, pl.ds(pl.multiple_of((slot * n + me) * pitch, 8), rows), :],
                 sums_sent.at[layer, t], sums_here.at[layer, t])

    def wait_sums(layer, t):
        wait_bytes(o_send.at[t], sums_here.at[layer, t])

    def wait_sums_sent(layer, t):
        wait_bytes(o_send.at[t, :, pl.ds(0, (n - 2 + layer) * rows), :], sums_sent.at[layer, t])

    def column(row):
        return jnp.broadcast_to(row.astype(F32), (LANES, row.shape[-1])).T

    def prepare_first(layer):
        for block in range(4):
            part = slice(block * channels, (block + 1) * channels)
            weight = w_proj_ref[layer, :, part].astype(F32).T.astype(BF16)
            bias = column(b_proj_ref[layer:layer + 1, part])
            for slot in range(slots):
                wp[layer, slot, block * n:(block + 1) * n] = weight[slot * n:(slot + 1) * n]
                bp[layer, slot, block * n:(block + 1) * n] = bias[slot * n:(slot + 1) * n]
        vec[layer, 0] = column(ln_in_ref[layer, 0:1])
        vec[layer, 1] = column(ln_in_ref[layer, 1:2])

    def prepare_rest(layer):
        wg[layer] = w_gate_ref[layer].astype(F32).T.astype(BF16)
        wo[layer] = w_out_ref[layer].astype(F32).T.astype(BF16)
        vec[layer, 2] = column(b_gate_ref[layer:layer + 1])
        vec[layer, 3] = column(ln_out_ref[layer, 0:1])
        vec[layer, 4] = column(ln_out_ref[layer, 1:2])
        vec[layer, 5] = column(b_out_ref[layer:layer + 1])

    def first_norm(t):
        def some(step):
            for k in range(group):
                i = step * group + k
                values = z_ref[i, lanes(t), :].astype(F32).T
                zt[i, :, lanes(t)] = values.astype(BF16)
                znt[i, :, lanes(t)] = norm_rows(values, vec[0, 0], vec[0, 1])

        loop(rows // group, some)

    def gated(layer, slot, pairs):
        normed = jnp.concatenate([znt[i, :, lanes(t)] for i, t in pairs], axis=1)
        projected = dot(wp[layer, slot], normed, ((1,), (0,)))
        bias = bp[layer, slot]
        for k, (i, t) in enumerate(pairs):
            part = projected[:, k * LANES:(k + 1) * LANES] + bias
            kept = keep[t, pl.ds(i, 1), :]
            stage_a[t, pl.ds(i, n, stride=pitch), :] = kept * jax.nn.sigmoid(part[n:2 * n]) * part[:n]
            stage_b[t, pl.ds(i, n, stride=pitch), :] = kept * jax.nn.sigmoid(part[3 * n:]) * part[2 * n:3 * n]

    def pack(slot, tile_list, unroll):
        def some(step):
            for k in range(unroll):
                d = step * unroll + k
                start = pl.multiple_of(d * pitch, 8)
                for t in tile_list:
                    ab_send[slot, d, 0, :, lanes(t)] = stage_a[t, pl.ds(start, rows), :].astype(BF16)
                    ab_send[slot, d, 1, :, lanes(t)] = stage_b[t, pl.ds(start, rows), :].astype(BF16)

        loop(n // unroll, some)

    def make_sides(layer, slot):
        loop(rows // 2, lambda step: gated(layer, slot, [(2 * step + k, t) for k in range(2) for t in range(tiles)]))
        pack(slot, range(tiles), 2)

    def make_sides_part(layer, slot, t):
        loop(rows // group, lambda step: gated(layer, slot, [(step * group + k, t) for k in range(group)]))
        pack(slot, [t], 8)

    def make_sides_half(layer, slot, t):
        loop(rows // 4, lambda step: gated(layer, slot, [(4 * step + k, t + j) for k in range(4) for j in range(2)]))
        pack(slot, [t, t + 1], 2)

    def make_gates(layer):
        def row(i):
            projected = dot(wg[layer], znt[i], ((1,), (0,)))
            for t in range(tiles):
                part = slice(t * LANES, (t + 1) * LANES)
                gate[i, :, part] = jax.nn.sigmoid(projected[:, part] + vec[layer, 2])

        loop(rows, row)

    def turn(layer, slot):
        if layer == 1:
            turned[...] = ab_recv[slot, 0].T

    def triangle(layer, slot, t):
        if layer == 0:
            for unit in range(2):
                part = slice(unit * half * rows, (unit + 1) * half * rows)
                o_send[t, slot, part] = dot(a_first[slot, part], b_first[slot, unit, lanes(t), :], ((1,), (1,)))
        else:
            o_send[t, slot] = dot(turned[...], ab_recv[slot, 1, :, lanes(t)], ((1,), (0,)))

    def finish(layer, t):
        def some(step):
            places = [step * group + k for k in range(group)]
            normed = [norm_rows(o_recv[t, pl.ds(i, channels, stride=pitch), :], vec[layer, 3], vec[layer, 4]) for i in places]
            update = dot(wo[layer], jnp.concatenate(normed, axis=1), ((1,), (0,)))
            for k, i in enumerate(places):
                added = update[:, k * LANES:(k + 1) * LANES] + vec[layer, 5]
                new = (zt[i, :, lanes(t)].astype(F32) + gate[i, :, lanes(t)] * added).astype(BF16)
                if layer == 0:
                    zt[i, :, lanes(t)] = new
                    znt[i, :, lanes(t)] = norm_rows(new.astype(F32), vec[1, 0], vec[1, 1])
                else:
                    out_ref[i, lanes(t), :] = new.astype(F32).T.astype(BF16)

        loop(rows // group, some)

    for copy in first_copies:
        copy.wait()
    prepare_first(0)
    for t in range(tiles):
        keep[t] = mask_ref[:, t * LANES:(t + 1) * LANES].astype(F32)

    def start(t):
        z_copy(t).wait()
        first_norm(t)
        make_sides_part(0, 0, t)
        make_sides_part(0, 1, t)

        @pl.when(t == 0)
        def _():
            pl.semaphore_wait(barrier, n - 1)

        send_first_sides(0, t, LANES)

    loop(tiles, start)
    for layer in range(2):
        def give_sides(step):
            wait_sides_sent(0, step + 1)
            make_sides(1, step + 1)
            loop(tiles, lambda t: send_sides(1, step + 1, t))

        def give_first_sums(step):
            for slot in couple_of(step):
                wait_twin(slot, twin_here)

            def some(t):
                for slot in couple_of(step):
                    triangle(0, slot, t)
                send_first_sums(step, t)

                @pl.when((t == tiles // 2 - 1) & (step < slots // 2 - 1))
                def _():
                    forward(step + 1)

            loop(tiles, some)

        def give_sums(slot):
            wait_sides(1, slot)
            turn(1, slot)

            def some(t):
                triangle(1, slot, t)
                send_sums(1, slot, t)

            loop(tiles, some)

        def take_sums(t):
            wait_sums(layer, t)
            finish(layer, t)
            if layer == 0:
                make_sides_part(1, 0, t)
                send_sides(1, 0, t)

        def forward(step):
            for slot in couple_of(step):
                wait_first_sides(slot)
            send_to_twin(step)

        if layer == 0:
            def give_first_sides(index):
                step, t = 1 + index // (tiles // 2), 2 * lax.rem(index, tiles // 2)
                for slot in couple_of(step):
                    make_sides_half(0, slot, t)
                send_first_sides(step, t, 2 * LANES)

                @pl.when(index == 1)
                def _():
                    forward(0)

            loop((slots // 2 - 1) * (tiles // 2), give_first_sides)
            for copy in rest_copies:
                copy.wait()
            prepare_rest(0)
            prepare_first(1)
            prepare_rest(1)
            make_gates(0)
            loop(slots // 2, give_first_sums)
            wait_sides_sent(0, 0)
        else:
            loop(slots - 1, give_sides)
            make_gates(1)
            loop(tiles, lambda t: wait_sums_sent(0, t))
            loop(slots, give_sums)
        loop(tiles, take_sums)

    loop(slots, lambda slot: wait_twin(slot, twin_sent))
    loop(slots, lambda slot: wait_sides_sent(1, slot))
    loop(tiles, lambda t: wait_sums_sent(1, t))


def solution(mesh):
    n = mesh.shape["dap"]
    side = math.isqrt(n // 2)
    row_spec = P(("batch", "dap"), None, None)
    mask_spec = P(("batch", "dap"), None)

    def local_layers(pair, *others):
        rows, cols, channels = pair.shape
        slots = channels // n
        tiles = cols // LANES
        pitch = rows + 8
        operands = (pair,) + others
        return pl.pallas_call(
            functools.partial(kernel, n, side, slots, pitch),
            out_shape=pltpu.VMEM(pair.shape, BF16),
            in_specs=[pl.BlockSpec(memory_space=pltpu.HBM)] * len(operands),
            out_specs=pl.BlockSpec(memory_space=pltpu.VMEM),
            scratch_shapes=[pltpu.VMEM(operand.shape, operand.dtype) for operand in operands] + [
                pltpu.SemaphoreType.DMA((tiles,)),
                pltpu.SemaphoreType.DMA((len(operands) - 1,)),
                pltpu.VMEM((slots, n, 2, rows, cols), BF16),
                pltpu.VMEM((slots, cols, cols), BF16),
                pltpu.VMEM((slots, 2, cols, cols), BF16),
                pltpu.VMEM((slots, 2, cols, cols), BF16),
                pltpu.VMEM((tiles, slots, cols, LANES), F32),
                pltpu.VMEM((tiles, channels * pitch, LANES), F32),
                pltpu.VMEM((tiles, n * pitch, LANES), F32),
                pltpu.VMEM((tiles, n * pitch, LANES), F32),
                pltpu.VMEM((cols, cols), BF16),
                pltpu.VMEM((rows, channels, cols), BF16),
                pltpu.VMEM((rows, channels, cols), BF16),
                pltpu.VMEM((rows, channels, cols), F32),
                pltpu.VMEM((2, slots, 4 * n, channels), BF16),
                pltpu.VMEM((2, slots, 4 * n, LANES), F32),
                pltpu.VMEM((2, channels, channels), BF16),
                pltpu.VMEM((2, channels, channels), BF16),
                pltpu.VMEM((2, 6, channels, LANES), F32),
                pltpu.VMEM((tiles, rows, LANES), F32),
                pltpu.SemaphoreType.DMA((2, slots)),
                pltpu.SemaphoreType.DMA((2, slots)),
                pltpu.SemaphoreType.DMA((2, tiles)),
                pltpu.SemaphoreType.DMA((2, tiles)),
                pltpu.SemaphoreType.DMA((slots,)),
                pltpu.SemaphoreType.DMA((slots,)),
            ],
            compiler_params=pltpu.CompilerParams(collective_id=0, has_side_effects=True, vmem_limit_bytes=54 * 2 ** 20),
            name="triangle_pair",
        )(*operands)

    return jax.shard_map(local_layers, mesh=mesh,
                         in_specs=(row_spec, mask_spec, P(), P(), P(), P(), P(), P(), P(), P()),
                         out_specs=row_spec, check_vma=False)
```
